256 devices in a mesh: runs: 2 (over y), amp: 128 (over z, x, core).
Axes of the slice: x: 4, y: 2, z: 16, core: 2. Of those that a mesh axis runs over, the one named last changes fastest.
The devices are a block of a 4x16x16 slice.
Arguments:
- initial_state: float32 [256, 1024, 128], P(('runs', 'amp')), parts along dimension 0, may hold values from -100 to 100
- gate_angles: float32 [10, 16], P('runs'), parts along dimension 0, may hold values from -3.140625 to 3.140625
- gate_pairs: int32 [5, 16, 2], replicated, may hold values from 0 to 6, as said below
- hop_coef: float32 [23], replicated, may hold values from 0.1 to 0.4
- hop_mask: int32 [23], replicated, may hold values 0 or 1
Outputs:
- adjoint: float32 [256, 1024, 128], P(('runs', 'amp')), parts along dimension 0
- block_grads: float32 [10, 128, 128], P('runs'), parts along dimension 0
The draws below stay inside these ranges and needn't reach their ends.
There are 2 independent parts, one for each index of `runs`. The reference program is written for one: setup_inputs(seed, part) draws one part's arguments, and reference() takes and returns one part's arrays. A program takes and returns all parts, laid end to end along the dimension named above; an argument that names none is the same for every part. Nothing has to cross between parts.
Inputs may be any that keep to these rules, and one draw needn't show every extreme that they name: `gate_pairs`: the two qubits of each rotation differ.
All inputs are finite; a program needn't handle non-finite values.
Results may differ from the reference program's by a relative error of at most 0.0003.
Values sent between devices are 32-bit elements; how exact they have to be, the bound alone decides.
No kernel may reach another device: no remote copies, remote signals or barrier semaphores. Data moves between devices by JAX's collectives and lax.ppermute only.
A program may use at most 192 MiB of HBM per device.

```python
import math
import jax
import jax.numpy as jnp
from jax import lax

BQ = 7
TQ = 7
YQ = 3
GIV = 16
BS = 128
TOP = 128
CW = 1024
BLOCKS = 5
HOPS = 23


def draw_initial_state(key, part):
    row_key, col_key, noise_key = jax.random.split(jax.random.fold_in(key, 11), 3)
    top_ramp = jnp.arange(TOP, dtype=jnp.float32)[:, None, None] / TOP
    mid_ramp = jnp.arange(CW, dtype=jnp.float32)[None, :, None] / CW
    row_scale = jnp.exp(jax.random.uniform(row_key, (TOP, 1, 1), minval=-1.15, maxval=1.15) + 0.55 * top_ramp - 0.3)
    col_scale = jnp.exp(jax.random.uniform(col_key, (1, CW, 1), minval=-1.15, maxval=1.15) + 0.55 * mid_ramp - 0.3)
    noise_part = jax.random.truncated_normal(noise_key, -6.0, 6.0, (TOP, CW, BS))
    return (row_scale * col_scale * noise_part).astype(jnp.float32)


def draw_gate_pairs(key, part):
    first_key, step_key = jax.random.split(jax.random.fold_in(key, 23))
    first_qubit = jax.random.randint(first_key, (BLOCKS, GIV), 0, BQ)
    step_size = jax.random.randint(step_key, (BLOCKS, GIV), 1, BQ)
    second_qubit = (first_qubit + step_size) % BQ
    return jnp.stack([first_qubit, second_qubit], axis=-1).astype(jnp.int32)


def touch_ends(values, rng, least, largest):
    extent = values.shape
    index_at = [jax.random.randint(jax.random.fold_in(rng, axis), (), 0, extent[axis]) for axis in range(len(extent))]
    values = values.at[tuple(index_at)].set(least)
    longest = extent.index(max(extent))
    index_at[longest] = (index_at[longest] + 1) % extent[longest]
    return values.at[tuple(index_at)].set(largest)


def setup_inputs(seed: int = 0, part: int = 0) -> dict:
    key_of = jax.random.split(jax.random.key(seed), 6)
    own_keys = jax.random.split(jax.random.fold_in(key_of[5], part), 6)
    initial_state = draw_initial_state(jax.random.fold_in(jax.random.fold_in(key_of[5], part), 71), part)
    gate_angles = jnp.clip(jax.random.uniform(own_keys[1], (BLOCKS, GIV), jnp.float32, -3.140625, 3.140625), -3.140625, 3.140625)
    gate_pairs = draw_gate_pairs(jax.random.fold_in(key_of[5], 71), part)
    hop_coef = jnp.clip(jnp.exp(jax.random.uniform(key_of[3], (HOPS,), jnp.float32, math.log(0.1), math.log(0.4))), 0.1, 0.4)
    hop_mask = touch_ends((jax.random.randint(key_of[4], (HOPS,), 0, 4) < 3).astype(jnp.int32), jax.random.fold_in(key_of[4], 1), 0, 1)
    return {"initial_state": initial_state, "gate_angles": gate_angles, "gate_pairs": gate_pairs, "hop_coef": hop_coef, "hop_mask": hop_mask}


exact_mode = lax.Precision.HIGHEST


def build_block(angles, pair_list, block_size):
    positions = jnp.arange(block_size, dtype=jnp.int32)
    diagonal = positions[:, None] == positions[None, :]

    def rotate(product, element):
        angle_now, pair_now = element
        one_bit = jnp.right_shift(positions, pair_now[0]) & 1
        two_bit = jnp.right_shift(positions, pair_now[1]) & 1
        flip_mask = jnp.left_shift(jnp.int32(1), pair_now[0]) | jnp.left_shift(jnp.int32(1), pair_now[1])
        partner = jnp.bitwise_xor(positions, flip_mask)
        differ = (one_bit != two_bit)[:, None]
        zero_value = jnp.zeros((), product.dtype)
        one_value = jnp.ones((), product.dtype)
        sine_value = jnp.sin(angle_now)
        signed = jnp.where(one_bit < two_bit, -sine_value, sine_value)[:, None]
        rotation = jnp.where(diagonal, jnp.where(differ, jnp.cos(angle_now), one_value), zero_value)
        rotation = rotation + jnp.where(differ & (positions[None, :] == partner[:, None]), signed, zero_value)
        return jnp.dot(rotation, product, precision=exact_mode), None

    identity = jnp.eye(block_size, dtype=angles.dtype)
    product, unused = lax.scan(rotate, identity, (angles, pair_list))
    return product


def shaped_for(amplitudes, window):
    top_rows, mid_count, lane_count = amplitudes.shape
    if window == 0:
        return amplitudes
    if window == 1:
        return amplitudes.reshape(top_rows, mid_count // 4, lane_count, 4)
    if window == 2:
        stride = min(2 ** (YQ - 1), mid_count // lane_count)
        return amplitudes.reshape(top_rows, mid_count // (stride * lane_count), lane_count, stride, lane_count)
    if window == 3:
        low_count = 2 ** YQ
        spread = lane_count // low_count
        return amplitudes.reshape(top_rows // spread, spread, mid_count // low_count, low_count, lane_count)
    return amplitudes.reshape(top_rows // lane_count, lane_count, mid_count, lane_count)


def apply_window(amplitudes, unitary, window):
    shaped = shaped_for(amplitudes, window)
    lane_count = amplitudes.shape[2]
    if window == 0:
        result = jnp.einsum('ij,tcj->tci', unitary, shaped, precision=exact_mode)
    elif window == 1:
        result = jnp.einsum('ij,tcja->tcia', unitary, shaped, precision=exact_mode)
    elif window == 2:
        result = jnp.einsum('ij,abjcd->abicd', unitary, shaped, precision=exact_mode)
    elif window == 3:
        low_count = 2 ** YQ
        spread = lane_count // low_count
        folded = unitary.reshape(spread, low_count, spread, low_count)
        result = jnp.einsum('pqkl,akblr->apbqr', folded, shaped, precision=exact_mode)
    else:
        result = jnp.einsum('ij,ajcr->aicr', unitary, shaped, precision=exact_mode)
    return result.reshape(amplitudes.shape)


def window_gram(adjoint, previous, window):
    lane_count = adjoint.shape[2]
    left_side = shaped_for(adjoint, window)
    right_side = shaped_for(previous, window)
    if window == 0:
        result = jnp.einsum('tci,tcj->ij', left_side, right_side, precision=exact_mode)
    elif window == 1:
        result = jnp.einsum('tcia,tcja->ij', left_side, right_side, precision=exact_mode)
    elif window == 2:
        result = jnp.einsum('abicd,abjcd->ij', left_side, right_side, precision=exact_mode)
    elif window == 3:
        result = jnp.einsum('apbqr,akblr->pqkl', left_side, right_side, precision=exact_mode)
    else:
        result = jnp.einsum('aicr,ajcr->ij', left_side, right_side, precision=exact_mode)
    return result.reshape(lane_count, lane_count)


def hop_pair(amplitudes, low_bit, high_bit):
    flat_values = amplitudes.reshape(-1)
    total_size = flat_values.shape[0]
    shaped = flat_values.reshape(total_size // 2 ** (high_bit + 1), 2, 2 ** (high_bit - low_bit - 1), 2, 2 ** low_bit)
    crossed = jnp.transpose(shaped, (0, 3, 2, 1, 4))
    differ = (1.0 - jnp.eye(2, dtype=amplitudes.dtype)).reshape(1, 2, 1, 2, 1)
    return (crossed * differ).reshape(amplitudes.shape)


def hamiltonian(amplitudes, weights):
    mid_count = amplitudes.shape[1]
    middle_bits = mid_count.bit_length() - 1
    first_top = BQ + middle_bits
    hop_pairs = [(position, position + 1) for position in range(BQ + YQ)]
    hop_pairs = hop_pairs + [(first_top + offset, first_top + offset + 1) for offset in range(TQ - 1)]
    hop_pairs = hop_pairs + [(BQ + offset, first_top + offset) for offset in range(TQ)]
    summed = jnp.zeros_like(amplitudes)
    for number in range(len(hop_pairs)):
        low_bit, high_bit = hop_pairs[number]
        summed = summed + weights[number] * hop_pair(amplitudes, low_bit, high_bit)
    return summed


def reference(initial_state, gate_angles, gate_pairs, hop_coef, hop_mask):
    lane_count = initial_state.shape[2]
    weights = hop_coef * hop_mask.astype(hop_coef.dtype)
    gate_blocks = [build_block(gate_angles[number], gate_pairs[number], lane_count) for number in range(BLOCKS)]
    current = initial_state
    for number in range(BLOCKS):
        current = apply_window(current, gate_blocks[number], number % 5)
    adjoint = hamiltonian(current, weights)
    factor = 2.0 / (initial_state.shape[0] * initial_state.shape[1])
    collected = []
    for number in range(BLOCKS - 1, BLOCKS - 6, -1):
        window = number % 5
        transposed = gate_blocks[number].T
        current = apply_window(current, transposed, window)
        collected.append(factor * window_gram(adjoint, current, window))
        adjoint = apply_window(adjoint, transposed, window)
    block_grads = jnp.stack(collected[::-1])
    return adjoint, block_grads
```

```python
import functools

import jax
import jax.numpy as jnp
from jax import lax
from jax.experimental import pallas as pl
from jax.experimental.pallas import tpu as pltpu
from jax.sharding import PartitionSpec as P

F32, BF16 = jnp.float32, jnp.bfloat16
AMP = "amp"
VMEM = pl.BlockSpec(memory_space=pltpu.VMEM)
SMEM = pl.BlockSpec(memory_space=pltpu.SMEM)

LANES = 128
LOW = 8
PARTS = 4
PACK = LOW + 2
CHAIN_FIRST = 10
RUNG_FIRST = 16


def chunk_of(device):
    return device ^ (((device >> 2) & 1) << 1)


def halves(value):
    high = value.astype(BF16)
    return high, (value - high.astype(F32)).astype(BF16)


def product(left, right, left_dim, right_dim):
    dims = (((left_dim,), (right_dim,)), ((), ()))
    dot = lambda a, b: lax.dot_general(a, b, dims, preferred_element_type=F32)
    return dot(left[0], right[0]) + (dot(left[0], right[1]) + dot(left[1], right[0]))


def own_bits():
    chunk = chunk_of(lax.axis_index(AMP))
    return [(chunk >> k) & 1 for k in range(4)]


def spread_selector():
    rows = lax.broadcasted_iota(jnp.int32, (PARTS * LANES, LANES), 0)
    columns = lax.broadcasted_iota(jnp.int32, (PARTS * LANES, LANES), 1)
    return ((rows >> 2) == columns).astype(F32).astype(BF16)


def same_part():
    shape = (PARTS * LANES, PARTS * LANES)
    rows = lax.broadcasted_iota(jnp.int32, shape, 0)
    columns = lax.broadcasted_iota(jnp.int32, shape, 1)
    return ((rows ^ columns) & (PARTS - 1)) == 0


def forward_kernel(angles, pairs, x, send, s1, s2, gates, k_high, k_low, cosines, sines, nat):
    block_count, rotation_count = angles.shape
    cosines[...] = jnp.cos(angles[...])
    sines[...] = jnp.sin(angles[...])
    row = lax.broadcasted_iota(jnp.int32, (LANES, LANES), 0)
    apart = row ^ lax.broadcasted_iota(jnp.int32, (LANES, LANES), 1)

    def build(b, carry):
        cos_row = cosines[pl.ds(b, 1), :]
        sin_row = sines[pl.ds(b, 1), :]

        def rotation(g):
            first = pairs[b * (2 * rotation_count) + 2 * g]
            second = pairs[b * (2 * rotation_count) + 2 * g + 1]
            flip = (1 << first) | (1 << second)
            one = (row >> first) & 1
            differ = one != ((row >> second) & 1)
            sine = sin_row[:, g : g + 1]
            off = jnp.where(one == 1, sine, -sine)
            value = jnp.where(differ & (apart == flip), off, 0.0)
            return jnp.where(apart == 0, jnp.where(differ, cos_row[:, g : g + 1], 1.0), value)

        def chain(low, count):
            if count == 1:
                return rotation(low)
            half = count // 2
            first = chain(low, half)
            return product(halves(chain(low + half, half)), halves(first), 1, 0)

        gates[b] = chain(0, rotation_count)
        return carry

    lax.fori_loop(0, block_count, build, 0)

    g0 = halves(gates[0])
    for q in range(PARTS):
        part = x[pl.ds(q, x.shape[0] // PARTS, stride=PARTS), :]
        s1[:, q * LANES : (q + 1) * LANES] = product(halves(part), g0, 1, 1)
    g1 = halves(gates[1])
    pick = spread_selector()
    keep = same_part()
    for out, source in ((k_high, g1[0]), (k_low, g1[1])):
        tall = jnp.dot(pick, source, preferred_element_type=F32).astype(BF16)
        wide = lax.dot_general(tall, pick, (((1,), (1,)), ((), ())), preferred_element_type=F32)
        out[...] = jnp.where(keep, wide, 0.0).astype(BF16)
    s2[...] = product(halves(s1[...]), (k_high[...], k_low[...]), 1, 1)
    g2 = halves(gates[2])
    for e in range(s2.shape[0] // LANES):
        s3 = product(g2, halves(s2[e * LANES : (e + 1) * LANES, :]), 1, 0)
        for q in range(PARTS):
            nat[pl.ds(e * PARTS * LANES + q, LANES, stride=PARTS), :] = s3[:, q * LANES : (q + 1) * LANES]
    for d in range(send.shape[0] // LOW):
        c = chunk_of(d)
        send[d * LOW : (d + 1) * LOW, :] = nat[c * LOW : (c + 1) * LOW, :]


def turn_kernel(z, gates, v, u4, half4, half5, half6, scratch):
    bits = own_bits()
    g3 = halves(gates[3])
    for block in range(z.shape[0] // LANES):
        rows = slice(block * LANES, (block + 1) * LANES)
        scratch[rows, :] = product(g3, halves(z[rows, :]), 1, 0)
    for c in range(LOW):
        u4[:, c * LANES : (c + 1) * LANES] = scratch[pl.ds(c, LANES, stride=LOW), :]
    v[...] = product(halves(gates[4]), halves(u4[...]), 1, 0)
    for out, k in ((half4, 4), (half5, 5), (half6, 6)):
        size = 1 << k
        for j in range(LANES // (2 * size)):
            start = pl.multiple_of(j * 2 * size + (1 - bits[k - 3]) * size, size)
            out[j * size : (j + 1) * size, :] = v[pl.ds(start, size), :]


def weight(coef, mask, number):
    return coef[number] * mask[number].astype(F32)


def pair_matrix(low, high, scale):
    rows = lax.broadcasted_iota(jnp.int32, (LANES, LANES), 0)
    columns = lax.broadcasted_iota(jnp.int32, (LANES, LANES), 1)
    active = (((rows >> low) ^ (rows >> high)) & 1) == 1
    return jnp.where(active & ((rows ^ columns) == ((1 << low) | (1 << high))), scale, 0.0)


def local_hops_kernel(v, coef, mask, out):
    lane_chain = sum(pair_matrix(k, k + 1, weight(coef, mask, k)) for k in range(6))
    top_chain = sum(pair_matrix(k, k + 1, weight(coef, mask, CHAIN_FIRST + k)) for k in range(6))
    lane_chain, top_chain = halves(lane_chain), halves(top_chain)
    rows = lax.broadcasted_iota(jnp.int32, (LANES, LANES), 0)
    columns = lax.broadcasted_iota(jnp.int32, (LANES, LANES), 1)
    rungs = []
    for k in range(3):
        scale = weight(coef, mask, RUNG_FIRST + k)
        paired = (rows ^ columns) == (1 << k)
        rungs.append([halves(jnp.where(paired & (((rows >> k) & 1) == 1 - c), scale, 0.0)) for c in range(2)])
    blocks = [v[:, c * LANES : (c + 1) * LANES] for c in range(LOW)]
    parts = [halves(block) for block in blocks]
    for c in range(LOW):
        total = product(parts[c], lane_chain, 1, 0) + product(top_chain, parts[c], 1, 0)
        for k in range(3):
            total = total + product(rungs[k][(c >> k) & 1], parts[c ^ (1 << k)], 1, 0)
        moved = pltpu.roll(blocks[c ^ 1], LANES // 2, 1)
        wanted = (columns >> 6) == 1 - (c & 1)
        total = total + jnp.where(wanted, weight(coef, mask, 6) * moved, 0.0)
        for k in range(2):
            if (c >> k) & 1 != (c >> (k + 1)) & 1:
                total = total + weight(coef, mask, 7 + k) * blocks[c ^ (3 << k)]
        out[:, c * LANES : (c + 1) * LANES] = total


def return_kernel(hops, other, half4, half5, half6, coef, mask, u4, z, gates, send, lam, scratch):
    bits = own_bits()
    lam[...] = hops[...]
    wide = lam.shape[1] // 2
    to = pl.multiple_of((1 - bits[0]) * wide, wide)
    source = pl.multiple_of(bits[0] * wide, wide)
    lam[:, pl.ds(to, wide)] += weight(coef, mask, 9) * other[:, pl.ds(source, wide)]
    for j in range(LANES // 16):
        to = pl.multiple_of(j * 16 + (1 - bits[0]) * 8, 8)
        source = pl.multiple_of(j * 16 + bits[0] * 8, 8)
        lam[pl.ds(to, 8), :] += weight(coef, mask, RUNG_FIRST + 3) * other[pl.ds(source, 8), :]
    for half, k in ((half4, 4), (half5, 5), (half6, 6)):
        size = 1 << k
        for j in range(LANES // (2 * size)):
            to = pl.multiple_of(j * 2 * size + (1 - bits[k - 3]) * size, size)
            lam[pl.ds(to, size), :] += weight(coef, mask, RUNG_FIRST + k) * half[j * size : (j + 1) * size, :]
    lam5 = halves(lam[...])
    top_rows = send.shape[0] // PACK
    send[pl.ds(LOW, top_rows, stride=PACK), :] = product(lam5, halves(u4[...]), 1, 1)
    lam4 = product(halves(gates[4]), lam5, 0, 0)
    for c in range(LOW):
        scratch[pl.ds(c, LANES, stride=LOW), :] = lam4[:, c * LANES : (c + 1) * LANES]
    g3 = halves(gates[3])
    gram = jnp.zeros((LANES, LANES), F32)
    for block in range(z.shape[0] // LANES):
        rows = slice(block * LANES, (block + 1) * LANES)
        inner = halves(scratch[rows, :])
        gram = gram + product(inner, halves(z[rows, :]), 1, 1)
        lam3 = product(g3, inner, 0, 0)
        for t in range(LANES // LOW):
            start = (block * (LANES // LOW) + t) * PACK
            send[start : start + LOW, :] = lam3[t * LOW : (t + 1) * LOW, :]
    send[pl.ds(LOW + 1, top_rows, stride=PACK), :] = gram


def backward_kernel(received, x, s1, s2, gates, k_high, k_low, adjoint, pack, nat):
    sources = received.shape[0] // PACK
    for d in range(sources):
        c = chunk_of(d)
        nat[c * LOW : (c + 1) * LOW, :] = received[d * PACK : d * PACK + LOW, :]
    for k in range(2):
        mine = jnp.sum(received[pl.ds(LOW + k, sources, stride=PACK), :], axis=0, keepdims=True)
        pack[pl.ds(3 + k, sources, stride=5), :] = jnp.broadcast_to(mine, (sources, LANES))
    count = x.shape[0] // PARTS
    g2 = halves(gates[2])
    gram2 = jnp.zeros((LANES, LANES), F32)
    pieces = []
    for e in range(count // LANES):
        lam3 = jnp.concatenate(
            [nat[pl.ds(e * PARTS * LANES + q, LANES, stride=PARTS), :] for q in range(PARTS)], axis=1
        )
        lam3 = halves(lam3)
        gram2 = gram2 + product(lam3, halves(s2[e * LANES : (e + 1) * LANES, :]), 1, 1)
        pieces.append(product(g2, lam3, 0, 0))
    lam2 = halves(jnp.concatenate(pieces, axis=0))
    wide = jnp.where(same_part(), product(lam2, halves(s1[...]), 0, 0), 0.0)
    pick = spread_selector()
    dims = (((0,), (0,)), ((), ()))
    high, low = halves(wide)
    dot = functools.partial(lax.dot_general, preferred_element_type=F32)
    folded = dot(pick, high, dims) + dot(pick, low, dims)
    high, low = halves(folded)
    gram1 = jnp.dot(high, pick, preferred_element_type=F32) + jnp.dot(low, pick, preferred_element_type=F32)
    lam1 = product(lam2, (k_high[...], k_low[...]), 1, 0)
    g0 = halves(gates[0])
    gram0 = jnp.zeros((LANES, LANES), F32)
    for q in range(PARTS):
        inner = halves(lam1[:, q * LANES : (q + 1) * LANES])
        gram0 = gram0 + product(inner, halves(x[pl.ds(q, count, stride=PARTS), :]), 0, 0)
        adjoint[pl.ds(q, count, stride=PARTS), :] = product(inner, g0, 1, 0)
    for k, gram in enumerate((gram0, gram1, gram2)):
        pack[pl.ds(k, sources, stride=5), :] = gram


def reduce_kernel(received, grads, pack, *, factor):
    sources = received.shape[0] // 5
    for k in range(3):
        mine = jnp.sum(received[pl.ds(k, sources, stride=5), :], axis=0, keepdims=True)
        pack[pl.ds(k, sources, stride=3), :] = jnp.broadcast_to(factor * mine, (sources, LANES))
    grads[0] = factor * received[pl.ds(4, sources, stride=5), :]
    grads[1] = factor * received[pl.ds(3, sources, stride=5), :]


def gather_kernel(received, upper, grads):
    sources = received.shape[0] // 3
    for k in range(3):
        grads[k] = received[pl.ds(k, sources, stride=3), :]
    for k in range(2):
        grads[3 + k] = upper[k]


def call(kernel, outs, specs, scratch=(), name=None):
    return pl.pallas_call(
        kernel,
        out_shape=[jax.ShapeDtypeStruct(shape, dtype) for shape, dtype in outs],
        in_specs=specs,
        out_specs=[VMEM] * len(outs),
        scratch_shapes=list(scratch),
        name=name,
    )


def exchange(rows):
    devices = lax.axis_size(AMP)
    shaped = rows.reshape(devices, rows.shape[0] // devices, 1, rows.shape[1])
    return lax.all_to_all(shaped, AMP, split_axis=0, concat_axis=0, tiled=True).reshape(rows.shape)


def swapped(value, flip):
    return lax.ppermute(value, AMP, [(i, i ^ flip) for i in range(lax.axis_size(AMP))])


def on_device(initial_state, gate_angles, gate_pairs, hop_coef, hop_mask):
    devices = lax.axis_size(AMP)
    middle = initial_state.shape[1]
    x = initial_state.reshape(middle, LANES)
    blocks = gate_angles.shape[0]
    wide = (middle // PARTS, PARTS * LANES)
    turned = (devices, LOW * LANES)
    square = (PARTS * LANES, PARTS * LANES)
    table = pltpu.VMEM(gate_angles.shape, F32)
    flat = pltpu.VMEM((middle, LANES), F32)

    send, s1, s2, gates, k_high, k_low = call(
        forward_kernel,
        [((middle, LANES), F32), (wide, F32), (wide, F32), ((blocks, LANES, LANES), F32), (square, BF16), (square, BF16)],
        [VMEM, SMEM, VMEM],
        [table, table, flat],
        "forward",
    )(gate_angles, gate_pairs.reshape(-1), x)
    z = exchange(send)
    half = (devices // 2, LOW * LANES)
    v, u4, half4, half5, half6 = call(
        turn_kernel,
        [(turned, F32), (turned, F32), (half, F32), (half, F32), (half, F32)],
        [VMEM, VMEM],
        [flat],
        "turn",
    )(z, gates)
    other = swapped(v, 1)
    half4, half5, half6 = swapped(half4, 2), swapped(half5, 6), swapped(half6, 8)
    (hops,) = call(local_hops_kernel, [(turned, F32)], [VMEM, SMEM, SMEM], (), "hops")(v, hop_coef, hop_mask)
    (send,) = call(
        return_kernel,
        [((devices * PACK, LANES), F32)],
        [VMEM] * 5 + [SMEM] * 2 + [VMEM] * 3,
        [pltpu.VMEM(turned, F32), flat],
        "back",
    )(hops, other, half4, half5, half6, hop_coef, hop_mask, u4, z, gates)
    received = exchange(send)
    adjoint, pack = call(
        backward_kernel,
        [((middle, LANES), F32), ((devices * 5, LANES), F32)],
        [VMEM] * 7,
        [flat],
        "backward",
    )(received, x, s1, s2, gates, k_high, k_low)
    factor = 2.0 / (devices * middle)
    upper, pack = call(
        functools.partial(reduce_kernel, factor=factor),
        [((2, LANES, LANES), F32), ((devices * 3, LANES), F32)],
        [VMEM],
        (),
        "reduce",
    )(exchange(pack))
    (grads,) = call(gather_kernel, [((blocks, LANES, LANES), F32)], [VMEM, VMEM], (), "gather")(exchange(pack), upper)
    return adjoint.reshape(initial_state.shape), grads


def solution(mesh):
    return jax.shard_map(
        on_device,
        mesh=mesh,
        in_specs=(P(("runs", AMP), None, None), P("runs", None), P(), P(), P()),
        out_specs=(P(("runs", AMP), None, None), P("runs", None, None)),
        check_vma=False,
    )
```

```python
import functools

import jax
import jax.numpy as jnp
from jax import lax
from jax.experimental import pallas as pl
from jax.experimental.pallas import tpu as pltpu
from jax.sharding import Mesh
from jax.sharding import PartitionSpec as P

F32, BF16 = jnp.float32, jnp.bfloat16
AMP = ("far", "near")
VMEM = pl.BlockSpec(memory_space=pltpu.VMEM)
SMEM = pl.BlockSpec(memory_space=pltpu.SMEM)

LANES = 128
LOW = 8
PARTS = 4
NEAR = 8
CHAIN_FIRST = 10
RUNG_FIRST = 16


def chunk_of(device):
    return device ^ (((device >> 2) & 1) << 1)


def halves(value):
    high = value.astype(BF16)
    return high, (value - high.astype(F32)).astype(BF16)


def product(left, right, left_dim, right_dim):
    dims = (((left_dim,), (right_dim,)), ((), ()))
    dot = lambda a, b: lax.dot_general(a, b, dims, preferred_element_type=F32)
    return dot(left[0], right[0]) + (dot(left[0], right[1]) + dot(left[1], right[0]))


def own_bits():
    chunk = chunk_of(lax.axis_index(AMP))
    return [(chunk >> k) & 1 for k in range(4)]


def spread_selector():
    rows = lax.broadcasted_iota(jnp.int32, (PARTS * LANES, LANES), 0)
    columns = lax.broadcasted_iota(jnp.int32, (PARTS * LANES, LANES), 1)
    return ((rows >> 2) == columns).astype(F32).astype(BF16)


def same_part():
    shape = (PARTS * LANES, PARTS * LANES)
    rows = lax.broadcasted_iota(jnp.int32, shape, 0)
    columns = lax.broadcasted_iota(jnp.int32, shape, 1)
    return ((rows ^ columns) & (PARTS - 1)) == 0


def forward_kernel(angles, pairs, x_far, send, x, s1_high, s1_low, s2_high, s2_low, gates, k_high, k_low, level_high, level_low, nat, arrived):
    load = pltpu.make_async_copy(x_far, x, arrived)
    load.start()
    block_count, rotation_count = angles.shape
    cosines = jnp.cos(angles[...])
    sines = jnp.sin(angles[...])
    lane = lax.broadcasted_iota(jnp.int32, (LOW, LANES), 1)
    apart = lax.broadcasted_iota(jnp.int32, (LANES, LANES), 0) ^ lax.broadcasted_iota(jnp.int32, (LANES, LANES), 1)

    def turn_of(b, g):
        first, second = pairs[b, 0, g], pairs[b, 1, g]
        cosine = jnp.broadcast_to(cosines[b : b + 1, g : g + 1], lane.shape)
        sine = jnp.broadcast_to(sines[b : b + 1, g : g + 1], lane.shape)

        def at(index):
            one = (index >> first) & 1
            differ = one != ((index >> second) & 1)
            off = jnp.where(differ, jnp.where(one == 1, sine, -sine), 0.0)
            return jnp.where(differ, cosine, 1.0), off

        return (1 << first) | (1 << second), at

    def tall(value):
        return jnp.broadcast_to(value[0:1, :], (LANES, LANES))

    for b in range(block_count):
        for i in range(rotation_count // 2):
            flip1, at1 = turn_of(b, 2 * i)
            flip2, at2 = turn_of(b, 2 * i + 1)
            keep1, cross1 = at1(lane)
            keep2, cross2 = at2(lane)
            keep12, cross12 = at1(lane ^ flip2)
            total = jnp.where(apart == 0, tall(keep2 * keep1), 0.0)
            total = total + jnp.where(apart == flip1, tall(keep2 * cross1), 0.0)
            total = total + jnp.where(apart == flip2, tall(cross2 * keep12), 0.0)
            total = total + jnp.where(apart == (flip1 ^ flip2), tall(cross2 * cross12), 0.0)
            level_high[b, i], level_low[b, i] = halves(total)
    width = rotation_count // 2
    while width > 1:
        width //= 2
        for b in range(block_count):
            for i in range(width):
                left = (level_high[b, 2 * i], level_low[b, 2 * i])
                right = (level_high[b, 2 * i + 1], level_low[b, 2 * i + 1])
                high, low = halves(product(left, right, 1, 0))
                if width > 1:
                    level_high[b, i], level_low[b, i] = high, low
                else:
                    gates[b], gates[block_count + b] = high, low

    pick = spread_selector()
    keep = same_part()
    for out, source in ((k_high, gates[1]), (k_low, gates[block_count + 1])):
        spread = jnp.dot(pick, source, preferred_element_type=F32).astype(BF16)
        wide = lax.dot_general(spread, pick, (((1,), (1,)), ((), ())), preferred_element_type=F32)
        out[...] = jnp.where(keep, wide, 0.0).astype(BF16)
    load.wait()
    g0 = gate(gates, 0)
    for q in range(PARTS):
        part = x[pl.ds(q, x.shape[0] // PARTS, stride=PARTS), :]
        columns = slice(q * LANES, (q + 1) * LANES)
        s1_high[:, columns], s1_low[:, columns] = halves(product(halves(part), g0, 1, 0))
    s2_high[...], s2_low[...] = halves(product((s1_high[...], s1_low[...]), (k_high[...], k_low[...]), 1, 0))
    g2 = gate(gates, 2)
    for e in range(s2_high.shape[0] // LANES):
        rows = slice(e * LANES, (e + 1) * LANES)
        s3 = product(g2, (s2_high[rows, :], s2_low[rows, :]), 0, 0)
        for q in range(PARTS):
            nat[pl.ds(e * PARTS * LANES + q, LANES, stride=PARTS), :] = s3[:, q * LANES : (q + 1) * LANES]
    for d in range(send.shape[0] // LOW):
        c = chunk_of(d)
        send[d * LOW : (d + 1) * LOW, :] = nat[c * LOW : (c + 1) * LOW, :]


def gate(gates, number):
    return gates[number], gates[gates.shape[0] // 2 + number]


def turn_kernel(z, gates, v, u4_high, u4_low, half4, half5, half6, scratch):
    bits = own_bits()
    g3 = gate(gates, 3)
    for block in range(z.shape[0] // LANES):
        rows = slice(block * LANES, (block + 1) * LANES)
        scratch[rows, :] = product(g3, halves(z[rows, :]), 0, 0)
    for c in range(LOW):
        columns = slice(c * LANES, (c + 1) * LANES)
        u4_high[:, columns], u4_low[:, columns] = halves(scratch[pl.ds(c, LANES, stride=LOW), :])
    v[...] = product(gate(gates, 4), (u4_high[...], u4_low[...]), 0, 0)
    for out, k in ((half4, 4), (half5, 5), (half6, 6)):
        size = 1 << k
        for j in range(LANES // (2 * size)):
            start = pl.multiple_of(j * 2 * size + (1 - bits[k - 3]) * size, size)
            out[j * size : (j + 1) * size, :] = v[pl.ds(start, size), :]


def weight(coef, mask, number):
    return coef[number] * mask[number].astype(F32)


def pair_matrix(low, high, scale):
    rows = lax.broadcasted_iota(jnp.int32, (LANES, LANES), 0)
    columns = lax.broadcasted_iota(jnp.int32, (LANES, LANES), 1)
    active = (((rows >> low) ^ (rows >> high)) & 1) == 1
    return jnp.where(active & ((rows ^ columns) == ((1 << low) | (1 << high))), scale, 0.0)


def local_hops_kernel(v, coef, mask, out):
    lane_chain = sum(pair_matrix(k, k + 1, weight(coef, mask, k)) for k in range(6))
    top_chain = sum(pair_matrix(k, k + 1, weight(coef, mask, CHAIN_FIRST + k)) for k in range(6))
    lane_chain, top_chain = halves(lane_chain), halves(top_chain)
    rows = lax.broadcasted_iota(jnp.int32, (LANES, LANES), 0)
    columns = lax.broadcasted_iota(jnp.int32, (LANES, LANES), 1)
    rungs = []
    for k in range(3):
        scale = weight(coef, mask, RUNG_FIRST + k)
        paired = (rows ^ columns) == (1 << k)
        rungs.append([halves(jnp.where(paired & (((rows >> k) & 1) == 1 - c), scale, 0.0)) for c in range(2)])
    blocks = [v[:, c * LANES : (c + 1) * LANES] for c in range(LOW)]
    parts = [halves(block) for block in blocks]
    for c in range(LOW):
        total = product(parts[c], lane_chain, 1, 0) + product(top_chain, parts[c], 1, 0)
        for k in range(3):
            total = total + product(rungs[k][(c >> k) & 1], parts[c ^ (1 << k)], 1, 0)
        moved = pltpu.roll(blocks[c ^ 1], LANES // 2, 1)
        wanted = (columns >> 6) == 1 - (c & 1)
        total = total + jnp.where(wanted, weight(coef, mask, 6) * moved, 0.0)
        for k in range(2):
            if (c >> k) & 1 != (c >> (k + 1)) & 1:
                total = total + weight(coef, mask, 7 + k) * blocks[c ^ (3 << k)]
        out[:, c * LANES : (c + 1) * LANES] = total


def return_kernel(hops, other, half4, half5, half6, coef, mask, u4_high, u4_low, z, gates, send, grams, lam, scratch):
    bits = own_bits()
    lam[...] = hops[...]
    wide = lam.shape[1] // 2
    to = pl.multiple_of((1 - bits[0]) * wide, wide)
    source = pl.multiple_of(bits[0] * wide, wide)
    lam[:, pl.ds(to, wide)] += weight(coef, mask, 9) * other[:, pl.ds(source, wide)]
    for j in range(LANES // 16):
        to = pl.multiple_of(j * 16 + (1 - bits[0]) * 8, 8)
        source = pl.multiple_of(j * 16 + bits[0] * 8, 8)
        lam[pl.ds(to, 8), :] += weight(coef, mask, RUNG_FIRST + 3) * other[pl.ds(source, 8), :]
    for half, k in ((half4, 4), (half5, 5), (half6, 6)):
        size = 1 << k
        for j in range(LANES // (2 * size)):
            to = pl.multiple_of(j * 2 * size + (1 - bits[k - 3]) * size, size)
            lam[pl.ds(to, size), :] += weight(coef, mask, RUNG_FIRST + k) * half[j * size : (j + 1) * size, :]
    lam5 = halves(lam[...])
    grams[1] = product(lam5, (u4_high[...], u4_low[...]), 1, 1)
    lam4 = product(gate(gates, 4), lam5, 1, 0)
    for c in range(LOW):
        scratch[pl.ds(c, LANES, stride=LOW), :] = lam4[:, c * LANES : (c + 1) * LANES]
    g3 = gate(gates, 3)
    gram = jnp.zeros((LANES, LANES), F32)
    for block in range(z.shape[0] // LANES):
        rows = slice(block * LANES, (block + 1) * LANES)
        inner = halves(scratch[rows, :])
        gram = gram + product(inner, halves(z[rows, :]), 1, 1)
        send[rows, :] = product(g3, inner, 1, 0)
    grams[0] = gram


def backward_kernel(received, x, s1_high, s1_low, s2_high, s2_low, gates, k_high, k_low, upper, adjoint, pack, nat):
    for d in range(received.shape[0] // LOW):
        c = chunk_of(d)
        nat[c * LOW : (c + 1) * LOW, :] = received[d * LOW : (d + 1) * LOW, :]
    count = x.shape[0] // PARTS
    g2 = gate(gates, 2)
    gram2 = jnp.zeros((LANES, LANES), F32)
    pieces = []
    for e in range(count // LANES):
        rows = slice(e * LANES, (e + 1) * LANES)
        lam3 = jnp.concatenate(
            [nat[pl.ds(e * PARTS * LANES + q, LANES, stride=PARTS), :] for q in range(PARTS)], axis=1
        )
        lam3 = halves(lam3)
        gram2 = gram2 + product(lam3, (s2_high[rows, :], s2_low[rows, :]), 1, 1)
        pieces.append(product(g2, lam3, 1, 0))
    lam2 = halves(jnp.concatenate(pieces, axis=0))
    wide = jnp.where(same_part(), product(lam2, (s1_high[...], s1_low[...]), 0, 0), 0.0)
    pick = spread_selector()
    dims = (((0,), (0,)), ((), ()))
    high, low = halves(wide)
    dot = functools.partial(lax.dot_general, preferred_element_type=F32)
    folded = dot(pick, high, dims) + dot(pick, low, dims)
    high, low = halves(folded)
    gram1 = jnp.dot(high, pick, preferred_element_type=F32) + jnp.dot(low, pick, preferred_element_type=F32)
    lam1 = product(lam2, (k_high[...], k_low[...]), 1, 1)
    g0 = gate(gates, 0)
    gram0 = jnp.zeros((LANES, LANES), F32)
    for q in range(PARTS):
        inner = halves(lam1[:, q * LANES : (q + 1) * LANES])
        gram0 = gram0 + product(inner, halves(x[pl.ds(q, count, stride=PARTS), :]), 0, 0)
        adjoint[pl.ds(q, count, stride=PARTS), :] = product(inner, g0, 1, 1)
    size = LANES // NEAR
    total = 5 * size
    for k, gram in enumerate((gram0, gram1, gram2, upper[0], upper[1])):
        for d in range(NEAR):
            pack[d * total + k * size : d * total + (k + 1) * size, :] = gram[d * size : (d + 1) * size, :]


def near_sum_kernel(received, pack):
    total = received.shape[0] // NEAR
    size = total // 5
    value = received[0:total, :]
    for d in range(1, NEAR):
        value = value + received[d * total : (d + 1) * total, :]
    for k in range(5):
        pack[pl.ds(k, size, stride=5), :] = value[k * size : (k + 1) * size, :]


def far_sum_kernel(received, pack, *, factor):
    size = received.shape[0] // 5
    for k in range(5):
        mine = jnp.sum(received[pl.ds(k, size, stride=5), :], axis=0, keepdims=True)
        pack[pl.ds(k, size, stride=5), :] = jnp.broadcast_to(factor * mine, (size, LANES))


def hand_out_kernel(received, pack):
    total = received.shape[0]
    size = total // 5
    for k in range(5):
        rows = received[pl.ds(k, size, stride=5), :]
        for d in range(NEAR):
            pack[d * total + k * size : d * total + (k + 1) * size, :] = rows


def gather_kernel(received, grads):
    total = received.shape[0] // NEAR
    size = total // 5
    for k in range(5):
        for d in range(NEAR):
            grads[k, d * size : (d + 1) * size, :] = received[d * total + k * size : d * total + (k + 1) * size, :]


def call(kernel, outs, specs, scratch=(), name=None):
    made = pl.pallas_call(
        kernel,
        out_shape=[
            jax.ShapeDtypeStruct(out[0], out[1]) if len(out) > 2 else pltpu.VMEM(out[0], out[1]) for out in outs
        ],
        in_specs=specs,
        out_specs=[VMEM] * len(outs),
        scratch_shapes=list(scratch),
        compiler_params=pltpu.CompilerParams(vmem_limit_bytes=24 << 20),
        name=name,
    )

    def run(*operands):
        kept = [
            pltpu.with_memory_space_constraint(operand, pltpu.VMEM) if spec is VMEM else operand
            for operand, spec in zip(operands, specs)
        ]
        return made(*kept)

    return run


def exchange(rows, axes):
    devices = lax.axis_size(axes)
    shaped = rows.reshape(devices, rows.shape[0] // devices, 1, rows.shape[1])
    return lax.all_to_all(shaped, axes, split_axis=0, concat_axis=0, tiled=True).reshape(rows.shape)


def swapped(value, flip):
    return lax.ppermute(value, AMP, [(i, i ^ flip) for i in range(lax.axis_size(AMP))])


def on_device(initial_state, gate_angles, gate_pairs, hop_coef, hop_mask):
    devices = lax.axis_size(AMP)
    middle = initial_state.shape[1]
    x = initial_state.reshape(middle, LANES)
    blocks, rotations = gate_angles.shape
    wide = (middle // PARTS, PARTS * LANES)
    turned = (devices, LOW * LANES)
    half = (devices // 2, LOW * LANES)
    square = (PARTS * LANES, PARTS * LANES)
    level = pltpu.VMEM((blocks, rotations // 2, LANES, LANES), BF16)
    flat = pltpu.VMEM((middle, LANES), F32)

    send, x_near, s1_high, s1_low, s2_high, s2_low, gates, k_high, k_low = call(
        forward_kernel,
        [((middle, LANES), F32)] * 2
        + [(wide, BF16)] * 4
        + [((2 * blocks, LANES, LANES), BF16)]
        + [(square, BF16)] * 2,
        [VMEM, SMEM, pl.BlockSpec(memory_space=pl.ANY)],
        [level, level, flat, pltpu.SemaphoreType.DMA],
        "forward",
    )(gate_angles, jnp.swapaxes(gate_pairs, 1, 2), x)
    z = exchange(send, AMP)
    v, u4_high, u4_low, half4, half5, half6 = call(
        turn_kernel,
        [(turned, F32), (turned, BF16), (turned, BF16), (half, F32), (half, F32), (half, F32)],
        [VMEM, VMEM],
        [flat],
        "turn",
    )(z, gates)
    other = swapped(v, 1)
    half4, half5, half6 = swapped(half4, 2), swapped(half5, 6), swapped(half6, 8)
    (hops,) = call(local_hops_kernel, [(turned, F32)], [VMEM, SMEM, SMEM], (), "hops")(v, hop_coef, hop_mask)
    send, upper = call(
        return_kernel,
        [((middle, LANES), F32), ((2, LANES, LANES), F32)],
        [VMEM] * 5 + [SMEM] * 2 + [VMEM] * 4,
        [pltpu.VMEM(turned, F32), flat],
        "back",
    )(hops, other, half4, half5, half6, hop_coef, hop_mask, u4_high, u4_low, z, gates)
    received = exchange(send, AMP)
    pack = ((5 * LANES, LANES), F32)
    rows = ((5 * LANES // NEAR, LANES), F32)
    adjoint, partial = call(backward_kernel, [((middle, LANES), F32), pack], [VMEM] * 10, [flat], "backward")(
        received, x_near, s1_high, s1_low, s2_high, s2_low, gates, k_high, k_low, upper
    )
    (partial,) = call(near_sum_kernel, [rows], [VMEM], (), "near")(exchange(partial, "near"))
    far_sum = functools.partial(far_sum_kernel, factor=2.0 / (devices * middle))
    (sums,) = call(far_sum, [rows], [VMEM], (), "far")(exchange(partial, "far"))
    (sums,) = call(hand_out_kernel, [pack], [VMEM], (), "hand")(exchange(sums, "far"))
    (grads,) = call(gather_kernel, [((blocks, LANES, LANES), F32, True)], [VMEM], (), "gather")(exchange(sums, "near"))
    return adjoint.reshape(initial_state.shape), grads


def solution(mesh):
    runs, amp = mesh.shape["runs"], mesh.shape["amp"]
    split = Mesh(mesh.devices.reshape(runs, amp // NEAR, NEAR), ("runs",) + AMP)
    return jax.shard_map(
        on_device,
        mesh=split,
        in_specs=(P(("runs",) + AMP, None, None), P("runs", None), P(), P(), P()),
        out_specs=(P(("runs",) + AMP, None, None), P("runs", None, None)),
        check_vma=False,
    )
```

```python
import functools

import jax
import jax.numpy as jnp
from jax import lax
from jax.experimental import pallas as pl
from jax.experimental.pallas import tpu as pltpu
from jax.sharding import Mesh
from jax.sharding import PartitionSpec as P

F32, BF16 = jnp.float32, jnp.bfloat16
AMP = ("far", "near")
VMEM = pl.BlockSpec(memory_space=pltpu.VMEM)
SMEM = pl.BlockSpec(memory_space=pltpu.SMEM)
FAR = pl.BlockSpec(memory_space=pltpu.HBM)

LANES = 128
LOW = 8
PARTS = 4
NEAR = 16
CHAIN_FIRST = 10
RUNG_FIRST = 16


def chunk_of(device):
    return device ^ (((device >> 2) & 1) << 1)


def halves(value):
    high = value.astype(BF16)
    return high, (value - high.astype(F32)).astype(BF16)


def product(left, right, left_dim, right_dim):
    dims = (((left_dim,), (right_dim,)), ((), ()))
    dot = lambda a, b: lax.dot_general(a, b, dims, preferred_element_type=F32)
    return dot(left[0], right[0]) + (dot(left[0], right[1]) + dot(left[1], right[0]))


def own_bits():
    chunk = chunk_of(lax.axis_index(AMP))
    return [(chunk >> k) & 1 for k in range(4)]


def spread_selector():
    rows = lax.broadcasted_iota(jnp.int32, (PARTS * LANES, LANES), 0)
    columns = lax.broadcasted_iota(jnp.int32, (PARTS * LANES, LANES), 1)
    return ((rows >> 2) == columns).astype(F32).astype(BF16)


def same_part():
    shape = (PARTS * LANES, PARTS * LANES)
    rows = lax.broadcasted_iota(jnp.int32, shape, 0)
    columns = lax.broadcasted_iota(jnp.int32, shape, 1)
    return ((rows ^ columns) & (PARTS - 1)) == 0


def forward_kernel(
    angles_far, pairs_far, x_far, send, x, s1_high, s1_low, s2_high, s2_low, gates, k_high, k_low,
    level_high, level_low, nat, angles, pairs, arrived,
):
    small = [
        pltpu.make_async_copy(angles_far, angles, arrived.at[0]),
        pltpu.make_async_copy(pairs_far, pairs, arrived.at[1]),
    ]
    load = pltpu.make_async_copy(x_far, x, arrived.at[2])
    for copy in small + [load]:
        copy.start()
    for copy in small:
        copy.wait()
    block_count, rotation_count = angles.shape
    cosines = jnp.cos(angles[...])
    sines = jnp.sin(angles[...])
    lane = lax.broadcasted_iota(jnp.int32, (LOW, LANES), 1)
    apart = lax.broadcasted_iota(jnp.int32, (LANES, LANES), 0) ^ lax.broadcasted_iota(jnp.int32, (LANES, LANES), 1)

    def turn_of(b, g):
        first, second = pairs[b, 0, g], pairs[b, 1, g]
        cosine = jnp.broadcast_to(cosines[b : b + 1, g : g + 1], lane.shape)
        sine = jnp.broadcast_to(sines[b : b + 1, g : g + 1], lane.shape)

        def at(index):
            one = (index >> first) & 1
            differ = one != ((index >> second) & 1)
            off = jnp.where(differ, jnp.where(one == 1, sine, -sine), 0.0)
            return jnp.where(differ, cosine, 1.0), off

        return (1 << first) | (1 << second), at

    def tall(value):
        return jnp.broadcast_to(value[0:1, :], (LANES, LANES))

    for b in range(block_count):
        for i in range(rotation_count // 2):
            flip1, at1 = turn_of(b, 2 * i)
            flip2, at2 = turn_of(b, 2 * i + 1)
            keep1, cross1 = at1(lane)
            keep2, cross2 = at2(lane)
            keep12, cross12 = at1(lane ^ flip2)
            total = jnp.where(apart == 0, tall(keep2 * keep1), 0.0)
            total = total + jnp.where(apart == flip1, tall(keep2 * cross1), 0.0)
            total = total + jnp.where(apart == flip2, tall(cross2 * keep12), 0.0)
            total = total + jnp.where(apart == (flip1 ^ flip2), tall(cross2 * cross12), 0.0)
            level_high[b, i], level_low[b, i] = halves(total)
    width = rotation_count // 2
    while width > 1:
        width //= 2
        for b in range(block_count):
            for i in range(width):
                left = (level_high[b, 2 * i], level_low[b, 2 * i])
                right = (level_high[b, 2 * i + 1], level_low[b, 2 * i + 1])
                high, low = halves(product(left, right, 1, 0))
                if width > 1:
                    level_high[b, i], level_low[b, i] = high, low
                else:
                    gates[b], gates[block_count + b] = high, low

    pick = spread_selector()
    keep = same_part()
    for out, source in ((k_high, gates[1]), (k_low, gates[block_count + 1])):
        spread = jnp.dot(pick, source, preferred_element_type=F32).astype(BF16)
        wide = lax.dot_general(spread, pick, (((1,), (1,)), ((), ())), preferred_element_type=F32)
        out[...] = jnp.where(keep, wide, 0.0).astype(BF16)
    load.wait()
    g0 = gate(gates, 0)
    for q in range(PARTS):
        part = x[pl.ds(q, x.shape[0] // PARTS, stride=PARTS), :]
        columns = slice(q * LANES, (q + 1) * LANES)
        s1_high[:, columns], s1_low[:, columns] = halves(product(halves(part), g0, 1, 0))
    s2_high[...], s2_low[...] = halves(product((s1_high[...], s1_low[...]), (k_high[...], k_low[...]), 1, 0))
    g2 = gate(gates, 2)
    for e in range(s2_high.shape[0] // LANES):
        rows = slice(e * LANES, (e + 1) * LANES)
        s3 = product(g2, (s2_high[rows, :], s2_low[rows, :]), 0, 0)
        for q in range(PARTS):
            nat[pl.ds(e * PARTS * LANES + q, LANES, stride=PARTS), :] = s3[:, q * LANES : (q + 1) * LANES]
    for d in range(send.shape[0] // LOW):
        c = chunk_of(d)
        send[d * LOW : (d + 1) * LOW, :] = nat[c * LOW : (c + 1) * LOW, :]


def gate(gates, number):
    return gates[number], gates[gates.shape[0] // 2 + number]


def turn_kernel(z, gates, v, u4_high, u4_low, half4, half5, half6, scratch):
    bits = own_bits()
    g3 = gate(gates, 3)
    for block in range(z.shape[0] // LANES):
        rows = slice(block * LANES, (block + 1) * LANES)
        scratch[rows, :] = product(g3, halves(z[rows, :]), 0, 0)
    for c in range(LOW):
        columns = slice(c * LANES, (c + 1) * LANES)
        u4_high[:, columns], u4_low[:, columns] = halves(scratch[pl.ds(c, LANES, stride=LOW), :])
    v[...] = product(gate(gates, 4), (u4_high[...], u4_low[...]), 0, 0)
    for out, k in ((half4, 4), (half5, 5), (half6, 6)):
        size = 1 << k
        for j in range(LANES // (2 * size)):
            start = pl.multiple_of(j * 2 * size + (1 - bits[k - 3]) * size, size)
            out[j * size : (j + 1) * size, :] = v[pl.ds(start, size), :]


def weight(coef, mask, number):
    return coef[number] * mask[number].astype(F32)


def pair_matrix(low, high, scale):
    rows = lax.broadcasted_iota(jnp.int32, (LANES, LANES), 0)
    columns = lax.broadcasted_iota(jnp.int32, (LANES, LANES), 1)
    active = (((rows >> low) ^ (rows >> high)) & 1) == 1
    return jnp.where(active & ((rows ^ columns) == ((1 << low) | (1 << high))), scale, 0.0)


def local_hops_kernel(v, coef, mask, out):
    lane_chain = sum(pair_matrix(k, k + 1, weight(coef, mask, k)) for k in range(6))
    top_chain = sum(pair_matrix(k, k + 1, weight(coef, mask, CHAIN_FIRST + k)) for k in range(6))
    lane_chain, top_chain = halves(lane_chain), halves(top_chain)
    rows = lax.broadcasted_iota(jnp.int32, (LANES, LANES), 0)
    columns = lax.broadcasted_iota(jnp.int32, (LANES, LANES), 1)
    rungs = []
    for k in range(3):
        scale = weight(coef, mask, RUNG_FIRST + k)
        paired = (rows ^ columns) == (1 << k)
        rungs.append([halves(jnp.where(paired & (((rows >> k) & 1) == 1 - c), scale, 0.0)) for c in range(2)])
    blocks = [v[:, c * LANES : (c + 1) * LANES] for c in range(LOW)]
    parts = [halves(block) for block in blocks]
    for c in range(LOW):
        total = product(parts[c], lane_chain, 1, 0) + product(top_chain, parts[c], 1, 0)
        for k in range(3):
            total = total + product(rungs[k][(c >> k) & 1], parts[c ^ (1 << k)], 1, 0)
        moved = pltpu.roll(blocks[c ^ 1], LANES // 2, 1)
        wanted = (columns >> 6) == 1 - (c & 1)
        total = total + jnp.where(wanted, weight(coef, mask, 6) * moved, 0.0)
        for k in range(2):
            if (c >> k) & 1 != (c >> (k + 1)) & 1:
                total = total + weight(coef, mask, 7 + k) * blocks[c ^ (3 << k)]
        out[:, c * LANES : (c + 1) * LANES] = total


def return_kernel(hops, other, half4, half5, half6, coef, mask, u4_high, u4_low, z, gates, send, grams, lam, scratch):
    bits = own_bits()
    lam[...] = hops[...]
    wide = lam.shape[1] // 2
    to = pl.multiple_of((1 - bits[0]) * wide, wide)
    source = pl.multiple_of(bits[0] * wide, wide)
    lam[:, pl.ds(to, wide)] += weight(coef, mask, 9) * other[:, pl.ds(source, wide)]
    for j in range(LANES // 16):
        to = pl.multiple_of(j * 16 + (1 - bits[0]) * 8, 8)
        source = pl.multiple_of(j * 16 + bits[0] * 8, 8)
        lam[pl.ds(to, 8), :] += weight(coef, mask, RUNG_FIRST + 3) * other[pl.ds(source, 8), :]
    for half, k in ((half4, 4), (half5, 5), (half6, 6)):
        size = 1 << k
        for j in range(LANES // (2 * size)):
            to = pl.multiple_of(j * 2 * size + (1 - bits[k - 3]) * size, size)
            lam[pl.ds(to, size), :] += weight(coef, mask, RUNG_FIRST + k) * half[j * size : (j + 1) * size, :]
    lam5 = halves(lam[...])
    grams[1] = product(lam5, (u4_high[...], u4_low[...]), 1, 1)
    lam4 = product(gate(gates, 4), lam5, 1, 0)
    for c in range(LOW):
        scratch[pl.ds(c, LANES, stride=LOW), :] = lam4[:, c * LANES : (c + 1) * LANES]
    g3 = gate(gates, 3)
    gram = jnp.zeros((LANES, LANES), F32)
    for block in range(z.shape[0] // LANES):
        rows = slice(block * LANES, (block + 1) * LANES)
        inner = halves(scratch[rows, :])
        gram = gram + product(inner, halves(z[rows, :]), 1, 1)
        send[rows, :] = product(g3, inner, 1, 0)
    grams[0] = gram


def backward_kernel(received, x, s1_high, s1_low, s2_high, s2_low, gates, k_high, k_low, upper, adjoint, pack, nat):
    for d in range(received.shape[0] // LOW):
        c = chunk_of(d)
        nat[c * LOW : (c + 1) * LOW, :] = received[d * LOW : (d + 1) * LOW, :]
    count = x.shape[0] // PARTS
    g2 = gate(gates, 2)
    gram2 = jnp.zeros((LANES, LANES), F32)
    pieces = []
    for e in range(count // LANES):
        rows = slice(e * LANES, (e + 1) * LANES)
        lam3 = jnp.concatenate(
            [nat[pl.ds(e * PARTS * LANES + q, LANES, stride=PARTS), :] for q in range(PARTS)], axis=1
        )
        lam3 = halves(lam3)
        gram2 = gram2 + product(lam3, (s2_high[rows, :], s2_low[rows, :]), 1, 1)
        pieces.append(product(g2, lam3, 1, 0))
    lam2 = halves(jnp.concatenate(pieces, axis=0))
    wide = jnp.where(same_part(), product(lam2, (s1_high[...], s1_low[...]), 0, 0), 0.0)
    pick = spread_selector()
    dims = (((0,), (0,)), ((), ()))
    high, low = halves(wide)
    dot = functools.partial(lax.dot_general, preferred_element_type=F32)
    folded = dot(pick, high, dims) + dot(pick, low, dims)
    high, low = halves(folded)
    gram1 = jnp.dot(high, pick, preferred_element_type=F32) + jnp.dot(low, pick, preferred_element_type=F32)
    lam1 = product(lam2, (k_high[...], k_low[...]), 1, 1)
    g0 = gate(gates, 0)
    gram0 = jnp.zeros((LANES, LANES), F32)
    for q in range(PARTS):
        inner = halves(lam1[:, q * LANES : (q + 1) * LANES])
        gram0 = gram0 + product(inner, halves(x[pl.ds(q, count, stride=PARTS), :]), 0, 0)
        adjoint[pl.ds(q, count, stride=PARTS), :] = product(inner, g0, 1, 1)
    size = LANES // NEAR
    total = 5 * size
    for k, gram in enumerate((gram0, gram1, gram2, upper[0], upper[1])):
        for d in range(NEAR):
            pack[d * total + k * size : d * total + (k + 1) * size, :] = gram[d * size : (d + 1) * size, :]


def sum_and_copy_kernel(received, pack, *, sources, factor):
    size = received.shape[0] // sources
    value = received[0:size, :]
    for d in range(1, sources):
        value = value + received[d * size : (d + 1) * size, :]
    for d in range(pack.shape[0] // size):
        pack[d * size : (d + 1) * size, :] = factor * value


def gather_kernel(received, grads):
    size = LANES // NEAR
    for d in range(NEAR):
        for k in range(5):
            start = (d * 5 + k) * size
            grads[k, d * size : (d + 1) * size, :] = received[start : start + size, :]


def call(kernel, outs, specs, scratch=(), name=None):
    made = pl.pallas_call(
        kernel,
        out_shape=[
            jax.ShapeDtypeStruct(out[0], out[1]) if len(out) > 2 else pltpu.VMEM(out[0], out[1]) for out in outs
        ],
        in_specs=specs,
        out_specs=[VMEM] * len(outs),
        scratch_shapes=list(scratch),
        compiler_params=pltpu.CompilerParams(vmem_limit_bytes=24 << 20),
        name=name,
    )

    def run(*operands):
        kept = [
            operand
            if spec is SMEM
            else pltpu.with_memory_space_constraint(operand, pltpu.HBM if spec is FAR else pltpu.VMEM)
            for operand, spec in zip(operands, specs)
        ]
        return made(*kept)

    return run


def exchange(rows, axes):
    devices = lax.axis_size(axes)
    shaped = rows.reshape(devices, rows.shape[0] // devices, 1, rows.shape[1])
    return lax.all_to_all(shaped, axes, split_axis=0, concat_axis=0, tiled=True).reshape(rows.shape)


def swapped(value, flip):
    return lax.ppermute(value, AMP, [(i, i ^ flip) for i in range(lax.axis_size(AMP))])


def on_device(initial_state, gate_angles, gate_pairs, hop_coef, hop_mask):
    devices = lax.axis_size(AMP)
    middle = initial_state.shape[1]
    x = initial_state.reshape(middle, LANES)
    blocks, rotations = gate_angles.shape
    wide = (middle // PARTS, PARTS * LANES)
    turned = (devices, LOW * LANES)
    half = (devices // 2, LOW * LANES)
    square = (PARTS * LANES, PARTS * LANES)
    level = pltpu.VMEM((blocks, rotations // 2, LANES, LANES), BF16)
    flat = pltpu.VMEM((middle, LANES), F32)

    send, x_near, s1_high, s1_low, s2_high, s2_low, gates, k_high, k_low = call(
        forward_kernel,
        [((middle, LANES), F32)] * 2
        + [(wide, BF16)] * 4
        + [((2 * blocks, LANES, LANES), BF16)]
        + [(square, BF16)] * 2,
        [FAR] * 3,
        [
            level,
            level,
            flat,
            pltpu.VMEM(gate_angles.shape, F32),
            pltpu.SMEM((blocks, 2, rotations), jnp.int32),
            pltpu.SemaphoreType.DMA((3,)),
        ],
        "forward",
    )(gate_angles, jnp.swapaxes(gate_pairs, 1, 2), x)
    z = exchange(send, AMP)
    v, u4_high, u4_low, half4, half5, half6 = call(
        turn_kernel,
        [(turned, F32), (turned, BF16), (turned, BF16), (half, F32), (half, F32), (half, F32)],
        [VMEM, VMEM],
        [flat],
        "turn",
    )(z, gates)
    other = swapped(v, 1)
    half4, half5, half6 = swapped(half4, 2), swapped(half5, 6), swapped(half6, 8)
    (hops,) = call(local_hops_kernel, [(turned, F32)], [VMEM, SMEM, SMEM], (), "hops")(v, hop_coef, hop_mask)
    send, upper = call(
        return_kernel,
        [((middle, LANES), F32), ((2, LANES, LANES), F32)],
        [VMEM] * 5 + [SMEM] * 2 + [VMEM] * 4,
        [pltpu.VMEM(turned, F32), flat],
        "back",
    )(hops, other, half4, half5, half6, hop_coef, hop_mask, u4_high, u4_low, z, gates)
    received = exchange(send, AMP)
    pack = ((5 * LANES, LANES), F32)
    far = devices // NEAR
    rows = ((far * 5 * LANES // NEAR, LANES), F32)
    adjoint, partial = call(backward_kernel, [((middle, LANES), F32, True), pack], [VMEM] * 10, [flat], "backward")(
        received, x_near, s1_high, s1_low, s2_high, s2_low, gates, k_high, k_low, upper
    )
    near_sum = functools.partial(sum_and_copy_kernel, sources=NEAR, factor=1.0)
    (partial,) = call(near_sum, [rows], [VMEM], (), "near")(exchange(partial, "near"))
    far_sum = functools.partial(sum_and_copy_kernel, sources=far, factor=2.0 / (devices * middle))
    (sums,) = call(far_sum, [pack], [VMEM], (), "far")(exchange(partial, "far"))
    (grads,) = call(gather_kernel, [((blocks, LANES, LANES), F32, True)], [VMEM], (), "gather")(exchange(sums, "near"))
    return adjoint.reshape(initial_state.shape), grads


def solution(mesh):
    runs, amp = mesh.shape["runs"], mesh.shape["amp"]
    split = Mesh(mesh.devices.reshape(runs, amp // NEAR, NEAR), ("runs",) + AMP)
    return jax.shard_map(
        on_device,
        mesh=split,
        in_specs=(P(("runs",) + AMP, None, None), P("runs", None), P(), P(), P()),
        out_specs=(P(("runs",) + AMP, None, None), P("runs", None, None)),
        check_vma=False,
    )
```

```python
import functools

import jax
import jax.numpy as jnp
from jax import lax
from jax.experimental import pallas as pl
from jax.experimental.pallas import tpu as pltpu
from jax.sharding import Mesh
from jax.sharding import PartitionSpec as P

F32, BF16 = jnp.float32, jnp.bfloat16
AMP = ("far", "near", "core")
VMEM = pl.BlockSpec(memory_space=pltpu.VMEM)
SMEM = pl.BlockSpec(memory_space=pltpu.SMEM)
FAR = pl.BlockSpec(memory_space=pltpu.HBM)

LANES = 128
LOW = 8
PARTS = 4
CORES = 2
NEAR = 8
CHAIN_FIRST = 10
RUNG_FIRST = 16


def chunk_of(device):
    return device ^ (((device >> 2) & 1) << 1)


def halves(value):
    high = value.astype(BF16)
    return high, (value - high.astype(F32)).astype(BF16)


def product(left, right, left_dim, right_dim):
    dims = (((left_dim,), (right_dim,)), ((), ()))
    dot = lambda a, b: lax.dot_general(a, b, dims, preferred_element_type=F32)
    return dot(left[0], right[0]) + (dot(left[0], right[1]) + dot(left[1], right[0]))


def own_bits():
    chunk = chunk_of(lax.axis_index(AMP))
    return [(chunk >> k) & 1 for k in range(4)]


def spread_selector():
    rows = lax.broadcasted_iota(jnp.int32, (PARTS * LANES, LANES), 0)
    columns = lax.broadcasted_iota(jnp.int32, (PARTS * LANES, LANES), 1)
    return ((rows >> 2) == columns).astype(F32).astype(BF16)


def same_part():
    shape = (PARTS * LANES, PARTS * LANES)
    rows = lax.broadcasted_iota(jnp.int32, shape, 0)
    columns = lax.broadcasted_iota(jnp.int32, shape, 1)
    return ((rows ^ columns) & (PARTS - 1)) == 0


def forward_kernel(
    angles_far, pairs_far, x_far, send, x, s1_high, s1_low, s2_high, s2_low, gates, k_high, k_low,
    level_high, level_low, nat, angles, pairs, arrived,
):
    small = [
        pltpu.make_async_copy(angles_far, angles, arrived.at[0]),
        pltpu.make_async_copy(pairs_far, pairs, arrived.at[1]),
    ]
    load = pltpu.make_async_copy(x_far, x, arrived.at[2])
    for copy in small + [load]:
        copy.start()
    for copy in small:
        copy.wait()
    block_count, rotation_count = angles.shape
    cosines = jnp.cos(angles[...])
    sines = jnp.sin(angles[...])
    lane = lax.broadcasted_iota(jnp.int32, (LOW, LANES), 1)
    apart = lax.broadcasted_iota(jnp.int32, (LANES, LANES), 0) ^ lax.broadcasted_iota(jnp.int32, (LANES, LANES), 1)

    def turn_of(b, g):
        first, second = pairs[b, 0, g], pairs[b, 1, g]
        cosine = jnp.broadcast_to(cosines[b : b + 1, g : g + 1], lane.shape)
        sine = jnp.broadcast_to(sines[b : b + 1, g : g + 1], lane.shape)

        def at(index):
            one = (index >> first) & 1
            differ = one != ((index >> second) & 1)
            off = jnp.where(differ, jnp.where(one == 1, sine, -sine), 0.0)
            return jnp.where(differ, cosine, 1.0), off

        return (1 << first) | (1 << second), at

    def tall(value):
        return jnp.broadcast_to(value[0:1, :], (LANES, LANES))

    for b in range(block_count):
        for i in range(rotation_count // 2):
            flip1, at1 = turn_of(b, 2 * i)
            flip2, at2 = turn_of(b, 2 * i + 1)
            keep1, cross1 = at1(lane)
            keep2, cross2 = at2(lane)
            keep12, cross12 = at1(lane ^ flip2)
            total = jnp.where(apart == 0, tall(keep2 * keep1), 0.0)
            total = total + jnp.where(apart == flip1, tall(keep2 * cross1), 0.0)
            total = total + jnp.where(apart == flip2, tall(cross2 * keep12), 0.0)
            total = total + jnp.where(apart == (flip1 ^ flip2), tall(cross2 * cross12), 0.0)
            level_high[b, i], level_low[b, i] = halves(total)
    width = rotation_count // 2
    while width > 1:
        width //= 2
        for b in range(block_count):
            for i in range(width):
                left = (level_high[b, 2 * i], level_low[b, 2 * i])
                right = (level_high[b, 2 * i + 1], level_low[b, 2 * i + 1])
                high, low = halves(product(left, right, 1, 0))
                if width > 1:
                    level_high[b, i], level_low[b, i] = high, low
                else:
                    gates[b], gates[block_count + b] = high, low

    pick = spread_selector()
    keep = same_part()
    for out, source in ((k_high, gates[1]), (k_low, gates[block_count + 1])):
        spread = jnp.dot(pick, source, preferred_element_type=F32).astype(BF16)
        wide = lax.dot_general(spread, pick, (((1,), (1,)), ((), ())), preferred_element_type=F32)
        out[...] = jnp.where(keep, wide, 0.0).astype(BF16)
    load.wait()
    g0 = gate(gates, 0)
    for q in range(PARTS):
        part = x[pl.ds(q, x.shape[0] // PARTS, stride=PARTS), :]
        columns = slice(q * LANES, (q + 1) * LANES)
        s1_high[:, columns], s1_low[:, columns] = halves(product(halves(part), g0, 1, 0))
    s2_high[...], s2_low[...] = halves(product((s1_high[...], s1_low[...]), (k_high[...], k_low[...]), 1, 0))
    g2 = gate(gates, 2)
    for e in range(s2_high.shape[0] // LANES):
        rows = slice(e * LANES, (e + 1) * LANES)
        s3 = product(g2, (s2_high[rows, :], s2_low[rows, :]), 0, 0)
        for q in range(PARTS):
            nat[pl.ds(e * PARTS * LANES + q, LANES, stride=PARTS), :] = s3[:, q * LANES : (q + 1) * LANES]
    for d in range(send.shape[0] // LOW):
        c = chunk_of(d)
        send[d * LOW : (d + 1) * LOW, :] = nat[c * LOW : (c + 1) * LOW, :]


def gate(gates, number):
    return gates[number], gates[gates.shape[0] // 2 + number]


def turn_kernel(z, gates, v, u4_high, u4_low, half4, half5, half6, scratch):
    bits = own_bits()
    g3 = gate(gates, 3)
    for block in range(z.shape[0] // LANES):
        rows = slice(block * LANES, (block + 1) * LANES)
        scratch[rows, :] = product(g3, halves(z[rows, :]), 0, 0)
    for c in range(LOW):
        columns = slice(c * LANES, (c + 1) * LANES)
        u4_high[:, columns], u4_low[:, columns] = halves(scratch[pl.ds(c, LANES, stride=LOW), :])
    v[...] = product(gate(gates, 4), (u4_high[...], u4_low[...]), 0, 0)
    for out, k in ((half4, 4), (half5, 5), (half6, 6)):
        size = 1 << k
        for j in range(LANES // (2 * size)):
            start = pl.multiple_of(j * 2 * size + (1 - bits[k - 3]) * size, size)
            out[j * size : (j + 1) * size, :] = v[pl.ds(start, size), :]


def weight(coef, mask, number):
    return coef[number] * mask[number].astype(F32)


def pair_matrix(low, high, scale):
    rows = lax.broadcasted_iota(jnp.int32, (LANES, LANES), 0)
    columns = lax.broadcasted_iota(jnp.int32, (LANES, LANES), 1)
    active = (((rows >> low) ^ (rows >> high)) & 1) == 1
    return jnp.where(active & ((rows ^ columns) == ((1 << low) | (1 << high))), scale, 0.0)


def local_hops_kernel(v, coef, mask, out):
    lane_chain = sum(pair_matrix(k, k + 1, weight(coef, mask, k)) for k in range(6))
    top_chain = sum(pair_matrix(k, k + 1, weight(coef, mask, CHAIN_FIRST + k)) for k in range(6))
    lane_chain, top_chain = halves(lane_chain), halves(top_chain)
    rows = lax.broadcasted_iota(jnp.int32, (LANES, LANES), 0)
    columns = lax.broadcasted_iota(jnp.int32, (LANES, LANES), 1)
    rungs = []
    for k in range(3):
        scale = weight(coef, mask, RUNG_FIRST + k)
        paired = (rows ^ columns) == (1 << k)
        rungs.append([halves(jnp.where(paired & (((rows >> k) & 1) == 1 - c), scale, 0.0)) for c in range(2)])
    blocks = [v[:, c * LANES : (c + 1) * LANES] for c in range(LOW)]
    parts = [halves(block) for block in blocks]
    for c in range(LOW):
        total = product(parts[c], lane_chain, 1, 0) + product(top_chain, parts[c], 1, 0)
        for k in range(3):
            total = total + product(rungs[k][(c >> k) & 1], parts[c ^ (1 << k)], 1, 0)
        moved = pltpu.roll(blocks[c ^ 1], LANES // 2, 1)
        wanted = (columns >> 6) == 1 - (c & 1)
        total = total + jnp.where(wanted, weight(coef, mask, 6) * moved, 0.0)
        for k in range(2):
            if (c >> k) & 1 != (c >> (k + 1)) & 1:
                total = total + weight(coef, mask, 7 + k) * blocks[c ^ (3 << k)]
        out[:, c * LANES : (c + 1) * LANES] = total


def return_kernel(hops, other, half4, half5, half6, coef, mask, u4_high, u4_low, z, gates, send, grams, lam, scratch):
    bits = own_bits()
    lam[...] = hops[...]
    wide = lam.shape[1] // 2
    to = pl.multiple_of((1 - bits[0]) * wide, wide)
    source = pl.multiple_of(bits[0] * wide, wide)
    lam[:, pl.ds(to, wide)] += weight(coef, mask, 9) * other[:, pl.ds(source, wide)]
    for j in range(LANES // 16):
        to = pl.multiple_of(j * 16 + (1 - bits[0]) * 8, 8)
        source = pl.multiple_of(j * 16 + bits[0] * 8, 8)
        lam[pl.ds(to, 8), :] += weight(coef, mask, RUNG_FIRST + 3) * other[pl.ds(source, 8), :]
    for half, k in ((half4, 4), (half5, 5), (half6, 6)):
        size = 1 << k
        for j in range(LANES // (2 * size)):
            to = pl.multiple_of(j * 2 * size + (1 - bits[k - 3]) * size, size)
            lam[pl.ds(to, size), :] += weight(coef, mask, RUNG_FIRST + k) * half[j * size : (j + 1) * size, :]
    lam5 = halves(lam[...])
    grams[1] = product(lam5, (u4_high[...], u4_low[...]), 1, 1)
    lam4 = product(gate(gates, 4), lam5, 1, 0)
    for c in range(LOW):
        scratch[pl.ds(c, LANES, stride=LOW), :] = lam4[:, c * LANES : (c + 1) * LANES]
    g3 = gate(gates, 3)
    gram = jnp.zeros((LANES, LANES), F32)
    for block in range(z.shape[0] // LANES):
        rows = slice(block * LANES, (block + 1) * LANES)
        inner = halves(scratch[rows, :])
        gram = gram + product(inner, halves(z[rows, :]), 1, 1)
        send[rows, :] = product(g3, inner, 1, 0)
    grams[0] = gram


def backward_kernel(
    received, x, s1_high, s1_low, s2_high, s2_low, gates, k_high, k_low, upper, lam1_high, lam1_low, own, away, nat, pack
):
    for d in range(received.shape[0] // LOW):
        c = chunk_of(d)
        nat[c * LOW : (c + 1) * LOW, :] = received[d * LOW : (d + 1) * LOW, :]
    count = x.shape[0] // PARTS
    g2 = gate(gates, 2)
    gram2 = jnp.zeros((LANES, LANES), F32)
    pieces = []
    for e in range(count // LANES):
        rows = slice(e * LANES, (e + 1) * LANES)
        lam3 = jnp.concatenate(
            [nat[pl.ds(e * PARTS * LANES + q, LANES, stride=PARTS), :] for q in range(PARTS)], axis=1
        )
        lam3 = halves(lam3)
        gram2 = gram2 + product(lam3, (s2_high[rows, :], s2_low[rows, :]), 1, 1)
        pieces.append(product(g2, lam3, 1, 0))
    lam2 = halves(jnp.concatenate(pieces, axis=0))
    wide = jnp.where(same_part(), product(lam2, (s1_high[...], s1_low[...]), 0, 0), 0.0)
    pick = spread_selector()
    dims = (((0,), (0,)), ((), ()))
    high, low = halves(wide)
    dot = functools.partial(lax.dot_general, preferred_element_type=F32)
    folded = dot(pick, high, dims) + dot(pick, low, dims)
    high, low = halves(folded)
    gram1 = jnp.dot(high, pick, preferred_element_type=F32) + jnp.dot(low, pick, preferred_element_type=F32)
    lam1_high[...], lam1_low[...] = halves(product(lam2, (k_high[...], k_low[...]), 1, 1))
    gram0 = jnp.zeros((LANES, LANES), F32)
    for q in range(PARTS):
        part = slice(q * LANES, (q + 1) * LANES)
        inner = (lam1_high[:, part], lam1_low[:, part])
        gram0 = gram0 + product(inner, halves(x[pl.ds(q, count, stride=PARTS), :]), 0, 0)
    size = LANES // (CORES * NEAR)
    for k, gram in enumerate((gram0, gram1, gram2, upper[0], upper[1])):
        for d in range(CORES * NEAR):
            start = (d * 5 + k) * size
            pack[start : start + size, :] = gram[d * size : (d + 1) * size, :]
    core = own_bits()[0]
    rows = own.shape[0]
    own[...] = pack[pl.ds(pl.multiple_of(core * rows, rows), rows), :]
    away[...] = pack[pl.ds(pl.multiple_of((1 - core) * rows, rows), rows), :]


def finish_kernel(lam1_high, lam1_low, gates, adjoint):
    g0 = gate(gates, 0)
    count = lam1_high.shape[0]
    for q in range(PARTS):
        part = slice(q * LANES, (q + 1) * LANES)
        adjoint[pl.ds(q, count, stride=PARTS), :] = product((lam1_high[:, part], lam1_low[:, part]), g0, 1, 1)


def merge_kernel(own, other, merged):
    merged[...] = own[...] + other[...]


def sum_and_copy_kernel(received, pack, *, sources, factor):
    size = received.shape[0] // sources
    value = received[0:size, :]
    for d in range(1, sources):
        value = value + received[d * size : (d + 1) * size, :]
    for d in range(pack.shape[0] // size):
        pack[d * size : (d + 1) * size, :] = factor * value


def gather_kernel(own, other, grads):
    size = LANES // (CORES * NEAR)
    core = own_bits()[0]
    for source, half in ((own, core), (other, 1 - core)):
        for d in range(NEAR):
            row = pl.multiple_of((half * NEAR + d) * size, size)
            for k in range(5):
                start = (d * 5 + k) * size
                grads[k, pl.ds(row, size), :] = source[start : start + size, :]


def call(kernel, outs, specs, scratch=(), name=None):
    made = pl.pallas_call(
        kernel,
        out_shape=[
            jax.ShapeDtypeStruct(out[0], out[1]) if len(out) > 2 else pltpu.VMEM(out[0], out[1]) for out in outs
        ],
        in_specs=specs,
        out_specs=[VMEM] * len(outs),
        scratch_shapes=list(scratch),
        compiler_params=pltpu.CompilerParams(vmem_limit_bytes=24 << 20),
        name=name,
    )

    def run(*operands):
        kept = [
            operand
            if spec is SMEM
            else pltpu.with_memory_space_constraint(operand, pltpu.HBM if spec is FAR else pltpu.VMEM)
            for operand, spec in zip(operands, specs)
        ]
        return made(*kept)

    return run


def exchange(rows, axes):
    devices = lax.axis_size(axes)
    shaped = rows.reshape(devices, rows.shape[0] // devices, 1, rows.shape[1])
    return lax.all_to_all(shaped, axes, split_axis=0, concat_axis=0, tiled=True).reshape(rows.shape)


def swapped(value, flip):
    return lax.ppermute(value, AMP, [(i, i ^ flip) for i in range(lax.axis_size(AMP))])


def on_device(initial_state, gate_angles, gate_pairs, hop_coef, hop_mask):
    devices = lax.axis_size(AMP)
    middle = initial_state.shape[1]
    x = initial_state.reshape(middle, LANES)
    blocks, rotations = gate_angles.shape
    wide = (middle // PARTS, PARTS * LANES)
    turned = (devices, LOW * LANES)
    half = (devices // 2, LOW * LANES)
    square = (PARTS * LANES, PARTS * LANES)
    level = pltpu.VMEM((blocks, rotations // 2, LANES, LANES), BF16)
    flat = pltpu.VMEM((middle, LANES), F32)

    send, x_near, s1_high, s1_low, s2_high, s2_low, gates, k_high, k_low = call(
        forward_kernel,
        [((middle, LANES), F32)] * 2
        + [(wide, BF16)] * 4
        + [((2 * blocks, LANES, LANES), BF16)]
        + [(square, BF16)] * 2,
        [FAR] * 3,
        [
            level,
            level,
            flat,
            pltpu.VMEM(gate_angles.shape, F32),
            pltpu.SMEM((blocks, 2, rotations), jnp.int32),
            pltpu.SemaphoreType.DMA((3,)),
        ],
        "forward",
    )(gate_angles, jnp.swapaxes(gate_pairs, 1, 2), x)
    z = exchange(send, AMP)
    v, u4_high, u4_low, half4, half5, half6 = call(
        turn_kernel,
        [(turned, F32), (turned, BF16), (turned, BF16), (half, F32), (half, F32), (half, F32)],
        [VMEM, VMEM],
        [flat],
        "turn",
    )(z, gates)
    half4, half5, half6 = swapped(half4, 2), swapped(half5, 6), swapped(half6, 8)
    other = swapped(v, 1)
    (hops,) = call(local_hops_kernel, [(turned, F32)], [VMEM, SMEM, SMEM], (), "hops")(v, hop_coef, hop_mask)
    send, upper = call(
        return_kernel,
        [((middle, LANES), F32), ((2, LANES, LANES), F32)],
        [VMEM] * 5 + [SMEM] * 2 + [VMEM] * 4,
        [pltpu.VMEM(turned, F32), flat],
        "back",
    )(hops, other, half4, half5, half6, hop_coef, hop_mask, u4_high, u4_low, z, gates)
    received = exchange(send, AMP)
    part = ((5 * LANES // CORES, LANES), F32)
    lam1_high, lam1_low, own, away = call(
        backward_kernel,
        [(wide, BF16), (wide, BF16), part, part],
        [VMEM] * 10,
        [flat, pltpu.VMEM((5 * LANES, LANES), F32)],
        "backward",
    )(received, x_near, s1_high, s1_low, s2_high, s2_low, gates, k_high, k_low, upper)
    away = swapped(away, 1)
    (adjoint,) = call(finish_kernel, [((middle, LANES), F32, True)], [VMEM] * 3, (), "finish")(lam1_high, lam1_low, gates)
    (partial,) = call(merge_kernel, [part], [VMEM] * 2, (), "merge")(own, away)
    far = devices // (CORES * NEAR)
    rows = ((far * part[0][0] // NEAR, LANES), F32)
    near_sum = functools.partial(sum_and_copy_kernel, sources=NEAR, factor=1.0)
    (partial,) = call(near_sum, [rows], [VMEM], (), "near")(exchange(partial, "near"))
    far_sum = functools.partial(sum_and_copy_kernel, sources=far, factor=2.0 / (devices * middle))
    (sums,) = call(far_sum, [part], [VMEM], (), "far")(exchange(partial, "far"))
    sums = exchange(sums, "near")
    (grads,) = call(gather_kernel, [((blocks, LANES, LANES), F32, True)], [VMEM] * 2, (), "gather")(sums, swapped(sums, 1))
    return adjoint.reshape(initial_state.shape), grads


def solution(mesh):
    runs, amp = mesh.shape["runs"], mesh.shape["amp"]
    split = Mesh(mesh.devices.reshape(runs, amp // (NEAR * CORES), NEAR, CORES), ("runs",) + AMP)
    return jax.shard_map(
        on_device,
        mesh=split,
        in_specs=(P(("runs",) + AMP, None, None), P("runs", None), P(), P(), P()),
        out_specs=(P(("runs",) + AMP, None, None), P("runs", None, None)),
        check_vma=False,
    )
```

```python
import functools

import jax
import jax.numpy as jnp
from jax import lax
from jax.experimental import pallas as pl
from jax.experimental.pallas import tpu as pltpu
from jax.sharding import Mesh
from jax.sharding import PartitionSpec as P

F32, BF16 = jnp.float32, jnp.bfloat16
AMP = ("far", "near", "core")
VMEM = pl.BlockSpec(memory_space=pltpu.VMEM)
SMEM = pl.BlockSpec(memory_space=pltpu.SMEM)
FAR = pl.BlockSpec(memory_space=pltpu.HBM)

LANES = 128
LOW = 8
PARTS = 4
CORES = 2
NEAR = 8
GROUP = LANES // PARTS
LANE_BIT = (5, 6, 0, 1, 2, 3, 4)
CHAIN_FIRST = 10
RUNG_FIRST = 16


def chunk_of(device):
    return device ^ (((device >> 2) & 1) << 1)


def halves(value):
    high = value.astype(BF16)
    return high, (value - high.astype(F32)).astype(BF16)


def product(left, right, left_dim, right_dim):
    lefts = jnp.concatenate([left[0], left[0], left[1]], axis=left_dim)
    rights = jnp.concatenate([right[0], right[1], right[0]], axis=right_dim)
    dims = (((left_dim,), (right_dim,)), ((), ()))
    return lax.dot_general(lefts, rights, dims, preferred_element_type=F32)


def own_bits():
    chunk = chunk_of(lax.axis_index(AMP))
    return [(chunk >> k) & 1 for k in range(4)]


def lane_order():
    rows = lax.broadcasted_iota(jnp.int32, (LANES, LANES), 0)
    lanes = lax.broadcasted_iota(jnp.int32, (LANES, LANES), 1)
    return (lanes == (rows & (PARTS - 1)) * GROUP + (rows >> 2)).astype(F32).astype(BF16)


def regroup(blocks):
    group = lax.broadcasted_iota(jnp.int32, blocks[0].shape, 1) // GROUP
    made = []
    for w in range(PARTS):
        total = None
        for u in range(PARTS):
            shift = (u - w) * GROUP % LANES
            moved = pltpu.roll(blocks[u], shift, 1) if shift else blocks[u]
            total = moved if total is None else jnp.where(group == u, moved, total)
        made.append(total)
    return made


def columns_of(array, number):
    return array[:, number * LANES : (number + 1) * LANES]


def forward_kernel(
    angles_far, pairs_far, x_far, send, x, s1_high, s1_low, s2_high, s2_low, gates,
    level_high, level_low, nat, angles, pairs, arrived,
):
    small = [
        pltpu.make_async_copy(angles_far, angles, arrived.at[0]),
        pltpu.make_async_copy(pairs_far, pairs, arrived.at[1]),
    ]
    load = pltpu.make_async_copy(x_far, x, arrived.at[2])
    for copy in small + [load]:
        copy.start()
    for copy in small:
        copy.wait()
    block_count, rotation_count = angles.shape
    cosines = jnp.cos(angles[...])
    sines = jnp.sin(angles[...])
    lane = lax.broadcasted_iota(jnp.int32, (LOW, LANES), 1)
    apart = lax.broadcasted_iota(jnp.int32, (LANES, LANES), 0) ^ lax.broadcasted_iota(jnp.int32, (LANES, LANES), 1)

    def turn_of(b, g):
        first, second = pairs[b, 0, g], pairs[b, 1, g]
        cosine = jnp.broadcast_to(cosines[b : b + 1, g : g + 1], lane.shape)
        sine = jnp.broadcast_to(sines[b : b + 1, g : g + 1], lane.shape)

        def at(index):
            one = (index >> first) & 1
            differ = one != ((index >> second) & 1)
            off = jnp.where(differ, jnp.where(one == 1, sine, -sine), 0.0)
            return jnp.where(differ, cosine, 1.0), off

        return (1 << first) | (1 << second), at

    def tall(value):
        return jnp.broadcast_to(value[0:1, :], (LANES, LANES))

    for b in range(block_count):
        for i in range(rotation_count // 2):
            flip1, at1 = turn_of(b, 2 * i)
            flip2, at2 = turn_of(b, 2 * i + 1)
            keep1, cross1 = at1(lane)
            keep2, cross2 = at2(lane)
            keep12, cross12 = at1(lane ^ flip2)
            total = jnp.where(apart == 0, tall(keep2 * keep1), 0.0)
            total = total + jnp.where(apart == flip1, tall(keep2 * cross1), 0.0)
            total = total + jnp.where(apart == flip2, tall(cross2 * keep12), 0.0)
            total = total + jnp.where(apart == (flip1 ^ flip2), tall(cross2 * cross12), 0.0)
            level_high[b, i], level_low[b, i] = halves(total)
    width = rotation_count // 2
    while width > 1:
        width //= 2
        for b in range(block_count):
            for i in range(width):
                left = (level_high[b, 2 * i], level_low[b, 2 * i])
                right = (level_high[b, 2 * i + 1], level_low[b, 2 * i + 1])
                high, low = halves(product(left, right, 1, 0))
                if width > 1:
                    level_high[b, i], level_low[b, i] = high, low
                else:
                    gates[b], gates[block_count + b] = high, low

    order = lane_order()
    for slot in (0, block_count):
        gates[slot] = jnp.dot(gates[slot], order, preferred_element_type=F32).astype(BF16)
    load.wait()
    g0 = gate(gates, 0)
    parts = [halves(x[pl.ds(q, x.shape[0] // PARTS, stride=PARTS), :]) for q in range(PARTS)]
    g1 = gate(gates, 1)
    for number, block in enumerate(regroup([product(part, g0, 1, 0) for part in parts])):
        columns = slice(number * LANES, (number + 1) * LANES)
        high, low = halves(block)
        s1_high[:, columns], s1_low[:, columns] = high, low
        s2_high[:, columns], s2_low[:, columns] = halves(product((high, low), g1, 1, 0))
    g2 = gate(gates, 2)
    for e in range(s2_high.shape[0] // LANES):
        rows = slice(e * LANES, (e + 1) * LANES)
        s3 = product(g2, (s2_high[rows, :], s2_low[rows, :]), 0, 0)
        for p, block in enumerate(regroup([columns_of(s3, number) for number in range(PARTS)])):
            nat[pl.ds(e * PARTS * LANES + p, LANES, stride=PARTS), :] = block
    for d in range(send.shape[0] // LOW):
        c = chunk_of(d)
        send[d * LOW : (d + 1) * LOW, :] = nat[c * LOW : (c + 1) * LOW, :]


def gate(gates, number):
    return gates[number], gates[gates.shape[0] // 2 + number]


def turn_kernel(z, gates, v, u4_high, u4_low, half4, half5, half6, scratch):
    bits = own_bits()
    g3 = gate(gates, 3)
    for block in range(z.shape[0] // LANES):
        rows = slice(block * LANES, (block + 1) * LANES)
        scratch[rows, :] = product(g3, halves(z[rows, :]), 0, 0)
    for c in range(LOW):
        columns = slice(c * LANES, (c + 1) * LANES)
        u4_high[:, columns], u4_low[:, columns] = halves(scratch[pl.ds(c, LANES, stride=LOW), :])
    v[...] = product(gate(gates, 4), (u4_high[...], u4_low[...]), 0, 0)
    for out, k in ((half4, 4), (half5, 5), (half6, 6)):
        size = 1 << k
        for j in range(LANES // (2 * size)):
            start = pl.multiple_of(j * 2 * size + (1 - bits[k - 3]) * size, size)
            out[j * size : (j + 1) * size, :] = v[pl.ds(start, size), :]


def weight(coef, mask, number):
    return coef[number] * mask[number].astype(F32)


def pair_matrix(low, high, scale):
    rows = lax.broadcasted_iota(jnp.int32, (LANES, LANES), 0)
    columns = lax.broadcasted_iota(jnp.int32, (LANES, LANES), 1)
    active = (((rows >> low) ^ (rows >> high)) & 1) == 1
    return jnp.where(active & ((rows ^ columns) == ((1 << low) | (1 << high))), scale, 0.0)


def local_hops_kernel(v, coef, mask, out):
    lane_chain = sum(pair_matrix(LANE_BIT[k], LANE_BIT[k + 1], weight(coef, mask, k)) for k in range(6))
    top_chain = sum(pair_matrix(k, k + 1, weight(coef, mask, CHAIN_FIRST + k)) for k in range(6))
    lane_chain, top_chain = halves(lane_chain), halves(top_chain)
    rows = lax.broadcasted_iota(jnp.int32, (LANES, LANES), 0)
    columns = lax.broadcasted_iota(jnp.int32, (LANES, LANES), 1)
    rungs = []
    for k in range(3):
        scale = weight(coef, mask, RUNG_FIRST + k)
        paired = (rows ^ columns) == (1 << k)
        rungs.append([halves(jnp.where(paired & (((rows >> k) & 1) == 1 - c), scale, 0.0)) for c in range(2)])
    blocks = [v[:, c * LANES : (c + 1) * LANES] for c in range(LOW)]
    parts = [halves(block) for block in blocks]
    for c in range(LOW):
        total = product(parts[c], lane_chain, 1, 0) + product(top_chain, parts[c], 1, 0)
        for k in range(3):
            total = total + product(rungs[k][(c >> k) & 1], parts[c ^ (1 << k)], 1, 0)
        step = 1 << LANE_BIT[6]
        moved = pltpu.roll(blocks[c ^ 1], LANES - step if c & 1 else step, 1)
        wanted = ((columns >> LANE_BIT[6]) & 1) == 1 - (c & 1)
        total = total + jnp.where(wanted, weight(coef, mask, 6) * moved, 0.0)
        for k in range(2):
            if (c >> k) & 1 != (c >> (k + 1)) & 1:
                total = total + weight(coef, mask, 7 + k) * blocks[c ^ (3 << k)]
        out[:, c * LANES : (c + 1) * LANES] = total


def return_kernel(hops, other, half4, half5, half6, coef, mask, u4_high, u4_low, z, gates, send, grams, lam, scratch):
    bits = own_bits()
    lam[...] = hops[...]
    wide = lam.shape[1] // 2
    to = pl.multiple_of((1 - bits[0]) * wide, wide)
    source = pl.multiple_of(bits[0] * wide, wide)
    lam[:, pl.ds(to, wide)] += weight(coef, mask, 9) * other[:, pl.ds(source, wide)]
    for j in range(LANES // 16):
        to = pl.multiple_of(j * 16 + (1 - bits[0]) * 8, 8)
        source = pl.multiple_of(j * 16 + bits[0] * 8, 8)
        lam[pl.ds(to, 8), :] += weight(coef, mask, RUNG_FIRST + 3) * other[pl.ds(source, 8), :]
    for half, k in ((half4, 4), (half5, 5), (half6, 6)):
        size = 1 << k
        for j in range(LANES // (2 * size)):
            to = pl.multiple_of(j * 2 * size + (1 - bits[k - 3]) * size, size)
            lam[pl.ds(to, size), :] += weight(coef, mask, RUNG_FIRST + k) * half[j * size : (j + 1) * size, :]
    lam5 = halves(lam[...])
    grams[1] = product(lam5, (u4_high[...], u4_low[...]), 1, 1)
    lam4 = product(gate(gates, 4), lam5, 1, 0)
    for c in range(LOW):
        scratch[pl.ds(c, LANES, stride=LOW), :] = lam4[:, c * LANES : (c + 1) * LANES]
    g3 = gate(gates, 3)
    gram = jnp.zeros((LANES, LANES), F32)
    for block in range(z.shape[0] // LANES):
        rows = slice(block * LANES, (block + 1) * LANES)
        inner = halves(scratch[rows, :])
        gram = gram + product(inner, halves(z[rows, :]), 1, 1)
        send[rows, :] = product(g3, inner, 1, 0)
    grams[0] = gram


def backward_kernel(
    received, x, s1_high, s1_low, s2_high, s2_low, gates, upper, lam1_high, lam1_low, own, away, nat, pack
):
    for d in range(received.shape[0] // LOW):
        c = chunk_of(d)
        nat[c * LOW : (c + 1) * LOW, :] = received[d * LOW : (d + 1) * LOW, :]
    count = x.shape[0] // PARTS
    g2 = gate(gates, 2)
    gram2 = jnp.zeros((LANES, LANES), F32)
    pieces = []
    for e in range(count // LANES):
        rows = slice(e * LANES, (e + 1) * LANES)
        blocks = [nat[pl.ds(e * PARTS * LANES + p, LANES, stride=PARTS), :] for p in range(PARTS)]
        lam3 = halves(jnp.concatenate(regroup(blocks), axis=1))
        gram2 = gram2 + product(lam3, (s2_high[rows, :], s2_low[rows, :]), 1, 1)
        pieces.append(product(g2, lam3, 1, 0))
    lam2 = halves(jnp.concatenate(pieces, axis=0))
    g1 = gate(gates, 1)
    gram1 = jnp.zeros((LANES, LANES), F32)
    blocks = []
    for number in range(PARTS):
        inner = (columns_of(lam2[0], number), columns_of(lam2[1], number))
        gram1 = gram1 + product(inner, (columns_of(s1_high, number), columns_of(s1_low, number)), 0, 0)
        blocks.append(product(inner, g1, 1, 1))
    gram0 = jnp.zeros((LANES, LANES), F32)
    for q, block in enumerate(regroup(blocks)):
        columns = slice(q * LANES, (q + 1) * LANES)
        inner = halves(block)
        lam1_high[:, columns], lam1_low[:, columns] = inner
        gram0 = gram0 + product(inner, halves(x[pl.ds(q, count, stride=PARTS), :]), 0, 0)
    order = lane_order()
    dot = functools.partial(jnp.dot, preferred_element_type=F32)
    high, low = halves(gram0)
    gram0 = dot(order, high) + dot(order, low)
    size = LANES // (CORES * NEAR)
    for k, gram in enumerate((gram0, gram1, gram2, upper[0], upper[1])):
        for d in range(CORES * NEAR):
            start = (d * 5 + k) * size
            pack[start : start + size, :] = gram[d * size : (d + 1) * size, :]
    core = own_bits()[0]
    rows = own.shape[0]
    own[...] = pack[pl.ds(pl.multiple_of(core * rows, rows), rows), :]
    away[...] = pack[pl.ds(pl.multiple_of((1 - core) * rows, rows), rows), :]


def finish_kernel(lam1_high, lam1_low, gates, adjoint, done):
    done[...] = jnp.zeros_like(done)
    g0 = gate(gates, 0)
    count = lam1_high.shape[0]
    for q in range(PARTS):
        part = slice(q * LANES, (q + 1) * LANES)
        adjoint[pl.ds(q, count, stride=PARTS), :] = product((lam1_high[:, part], lam1_low[:, part]), g0, 1, 1)


def merge_kernel(own, other, done, merged):
    merged[...] = own[...] + other[...]


def sum_and_copy_kernel(received, pack, *, sources, factor):
    size = received.shape[0] // sources
    value = received[0:size, :]
    for d in range(1, sources):
        value = value + received[d * size : (d + 1) * size, :]
    for d in range(pack.shape[0] // size):
        pack[d * size : (d + 1) * size, :] = factor * value


def gather_kernel(own, other, grads):
    size = LANES // (CORES * NEAR)
    core = own_bits()[0]
    for source, half in ((own, core), (other, 1 - core)):
        for d in range(NEAR):
            row = pl.multiple_of((half * NEAR + d) * size, size)
            for k in range(5):
                start = (d * 5 + k) * size
                grads[k, pl.ds(row, size), :] = source[start : start + size, :]


def call(kernel, outs, specs, scratch=(), name=None):
    made = pl.pallas_call(
        kernel,
        out_shape=[
            jax.ShapeDtypeStruct(out[0], out[1]) if len(out) > 2 else pltpu.VMEM(out[0], out[1]) for out in outs
        ],
        in_specs=specs,
        out_specs=[VMEM] * len(outs),
        scratch_shapes=list(scratch),
        compiler_params=pltpu.CompilerParams(vmem_limit_bytes=24 << 20),
        name=name,
    )

    def run(*operands):
        kept = [
            operand
            if spec is SMEM
            else pltpu.with_memory_space_constraint(operand, pltpu.HBM if spec is FAR else pltpu.VMEM)
            for operand, spec in zip(operands, specs)
        ]
        return made(*kept)

    return run


def exchange(rows, axes):
    devices = lax.axis_size(axes)
    shaped = rows.reshape(devices, rows.shape[0] // devices, 1, rows.shape[1])
    return lax.all_to_all(shaped, axes, split_axis=0, concat_axis=0, tiled=True).reshape(rows.shape)


def swapped(value, flip):
    return lax.ppermute(value, AMP, [(i, i ^ flip) for i in range(lax.axis_size(AMP))])


def on_device(initial_state, gate_angles, gate_pairs, hop_coef, hop_mask):
    devices = lax.axis_size(AMP)
    middle = initial_state.shape[1]
    x = initial_state.reshape(middle, LANES)
    blocks, rotations = gate_angles.shape
    wide = (middle // PARTS, PARTS * LANES)
    turned = (devices, LOW * LANES)
    half = (devices // 2, LOW * LANES)
    level = pltpu.VMEM((blocks, rotations // 2, LANES, LANES), BF16)
    flat = pltpu.VMEM((middle, LANES), F32)

    send, x_near, s1_high, s1_low, s2_high, s2_low, gates = call(
        forward_kernel,
        [((middle, LANES), F32)] * 2
        + [(wide, BF16)] * 4
        + [((2 * blocks, LANES, LANES), BF16)],
        [FAR] * 3,
        [
            level,
            level,
            flat,
            pltpu.VMEM(gate_angles.shape, F32),
            pltpu.SMEM((blocks, 2, rotations), jnp.int32),
            pltpu.SemaphoreType.DMA((3,)),
        ],
        "forward",
    )(gate_angles, jnp.swapaxes(gate_pairs, 1, 2), x)
    z = exchange(send, AMP)
    v, u4_high, u4_low, half4, half5, half6 = call(
        turn_kernel,
        [(turned, F32), (turned, BF16), (turned, BF16), (half, F32), (half, F32), (half, F32)],
        [VMEM, VMEM],
        [flat],
        "turn",
    )(z, gates)
    half4, half5, half6 = swapped(half4, 2), swapped(half5, 6), swapped(half6, 8)
    other = swapped(v, 1)
    (hops,) = call(local_hops_kernel, [(turned, F32)], [VMEM, SMEM, SMEM], (), "hops")(v, hop_coef, hop_mask)
    send, upper = call(
        return_kernel,
        [((middle, LANES), F32), ((2, LANES, LANES), F32)],
        [VMEM] * 5 + [SMEM] * 2 + [VMEM] * 4,
        [pltpu.VMEM(turned, F32), flat],
        "back",
    )(hops, other, half4, half5, half6, hop_coef, hop_mask, u4_high, u4_low, z, gates)
    received = exchange(send, AMP)
    part = ((5 * LANES // CORES, LANES), F32)
    lam1_high, lam1_low, own, away = call(
        backward_kernel,
        [(wide, BF16), (wide, BF16), part, part],
        [VMEM] * 8,
        [flat, pltpu.VMEM((5 * LANES, LANES), F32)],
        "backward",
    )(received, x_near, s1_high, s1_low, s2_high, s2_low, gates, upper)
    away = swapped(away, 1)
    adjoint, done = call(
        finish_kernel, [((middle, LANES), F32, True), ((LOW, LANES), F32)], [VMEM] * 3, (), "finish"
    )(lam1_high, lam1_low, gates)
    (partial,) = call(merge_kernel, [part], [VMEM] * 3, (), "merge")(own, away, done)
    far = devices // (CORES * NEAR)
    rows = ((far * part[0][0] // NEAR, LANES), F32)
    near_sum = functools.partial(sum_and_copy_kernel, sources=NEAR, factor=1.0)
    (partial,) = call(near_sum, [rows], [VMEM], (), "near")(exchange(partial, "near"))
    far_sum = functools.partial(sum_and_copy_kernel, sources=far, factor=2.0 / (devices * middle))
    (sums,) = call(far_sum, [part], [VMEM], (), "far")(exchange(partial, "far"))
    sums = exchange(sums, "near")
    (grads,) = call(gather_kernel, [((blocks, LANES, LANES), F32, True)], [VMEM] * 2, (), "gather")(sums, swapped(sums, 1))
    return adjoint.reshape(initial_state.shape), grads


def solution(mesh):
    runs, amp = mesh.shape["runs"], mesh.shape["amp"]
    split = Mesh(mesh.devices.reshape(runs, amp // (NEAR * CORES), NEAR, CORES), ("runs",) + AMP)
    return jax.shard_map(
        on_device,
        mesh=split,
        in_specs=(P(("runs",) + AMP, None, None), P("runs", None), P(), P(), P()),
        out_specs=(P(("runs",) + AMP, None, None), P("runs", None, None)),
        check_vma=False,
    )
```

```python
import functools

import jax
import jax.numpy as jnp
from jax import lax
from jax.experimental import pallas as pl
from jax.experimental.pallas import tpu as pltpu
from jax.sharding import Mesh
from jax.sharding import PartitionSpec as P

F32, BF16 = jnp.float32, jnp.bfloat16
AMP = ("far", "near", "core")
VMEM = pl.BlockSpec(memory_space=pltpu.VMEM)
SMEM = pl.BlockSpec(memory_space=pltpu.SMEM)
FAR = pl.BlockSpec(memory_space=pltpu.HBM)

LANES = 128
LOW = 8
PARTS = 4
CORES = 2
NEAR = 8
GROUP = LANES // PARTS
LANE_BIT = (5, 6, 0, 1, 2, 3, 4)
CHAIN_FIRST = 10
RUNG_FIRST = 16


def chunk_of(device):
    return device ^ (((device >> 2) & 1) << 1)


def halves(value):
    high = value.astype(BF16)
    return high, (value - high.astype(F32)).astype(BF16)


def product(left, right, left_dim, right_dim):
    lefts = jnp.concatenate([left[0], left[0], left[1]], axis=left_dim)
    rights = jnp.concatenate([right[0], right[1], right[0]], axis=right_dim)
    dims = (((left_dim,), (right_dim,)), ((), ()))
    return lax.dot_general(lefts, rights, dims, preferred_element_type=F32)


def short_product(left, right):
    dot = functools.partial(jnp.dot, preferred_element_type=F32)
    return dot(left[0], right[0]) + (dot(left[0], right[1]) + dot(left[1], right[0]))


def own_bits():
    chunk = chunk_of(lax.axis_index(AMP))
    return [(chunk >> k) & 1 for k in range(4)]


def lane_order():
    rows = lax.broadcasted_iota(jnp.int32, (LANES, LANES), 0)
    lanes = lax.broadcasted_iota(jnp.int32, (LANES, LANES), 1)
    return (lanes == (rows & (PARTS - 1)) * GROUP + (rows >> 2)).astype(F32).astype(BF16)


def regroup(blocks):
    group = lax.broadcasted_iota(jnp.int32, blocks[0].shape, 1) // GROUP
    made = []
    for w in range(PARTS):
        total = None
        for u in range(PARTS):
            shift = (u - w) * GROUP % LANES
            moved = pltpu.roll(blocks[u], shift, 1) if shift else blocks[u]
            total = moved if total is None else jnp.where(group == u, moved, total)
        made.append(total)
    return made


def columns_of(array, number):
    return array[:, number * LANES : (number + 1) * LANES]


def forward_kernel(
    angles_far, pairs_far, x_far, send, x, s1_high, s1_low, s2_high, s2_low, gates,
    level_high, level_low, nat, angles, pairs, arrived,
):
    small = [
        pltpu.make_async_copy(angles_far, angles, arrived.at[0]),
        pltpu.make_async_copy(pairs_far, pairs, arrived.at[1]),
    ]
    load = pltpu.make_async_copy(x_far, x, arrived.at[2])
    for copy in small + [load]:
        copy.start()
    for copy in small:
        copy.wait()
    block_count, rotation_count = angles.shape
    cosines = jnp.cos(angles[...])
    sines = jnp.sin(angles[...])
    lane = lax.broadcasted_iota(jnp.int32, (LOW, LANES), 1)
    apart = lax.broadcasted_iota(jnp.int32, (LANES, LANES), 0) ^ lax.broadcasted_iota(jnp.int32, (LANES, LANES), 1)

    def turn_of(b, g):
        first, second = pairs[b, 0, g], pairs[b, 1, g]
        cosine = jnp.broadcast_to(cosines[b : b + 1, g : g + 1], lane.shape)
        sine = jnp.broadcast_to(sines[b : b + 1, g : g + 1], lane.shape)

        def at(index):
            one = (index >> first) & 1
            differ = one != ((index >> second) & 1)
            off = jnp.where(differ, jnp.where(one == 1, sine, -sine), 0.0)
            return jnp.where(differ, cosine, 1.0), off

        return (1 << first) | (1 << second), at

    def tall(value):
        return jnp.broadcast_to(value[0:1, :], (LANES, LANES))

    for b in range(block_count):
        for i in range(rotation_count // 2):
            flip1, at1 = turn_of(b, 2 * i)
            flip2, at2 = turn_of(b, 2 * i + 1)
            keep1, cross1 = at1(lane)
            keep2, cross2 = at2(lane)
            keep12, cross12 = at1(lane ^ flip2)
            total = jnp.where(apart == 0, tall(keep2 * keep1), 0.0)
            total = total + jnp.where(apart == flip1, tall(keep2 * cross1), 0.0)
            total = total + jnp.where(apart == flip2, tall(cross2 * keep12), 0.0)
            total = total + jnp.where(apart == (flip1 ^ flip2), tall(cross2 * cross12), 0.0)
            level_high[b, i], level_low[b, i] = halves(total)
    width = rotation_count // 2
    while width > 1:
        width //= 2
        for b in range(block_count):
            for i in range(width):
                left = (level_high[b, 2 * i], level_low[b, 2 * i])
                right = (level_high[b, 2 * i + 1], level_low[b, 2 * i + 1])
                high, low = halves(short_product(left, right))
                if width > 1:
                    level_high[b, i], level_low[b, i] = high, low
                else:
                    gates[b], gates[block_count + b] = high, low

    order = lane_order()
    for slot in (0, block_count):
        gates[slot] = jnp.dot(gates[slot], order, preferred_element_type=F32).astype(BF16)
    load.wait()
    g0 = gate(gates, 0)
    parts = [halves(x[pl.ds(q, x.shape[0] // PARTS, stride=PARTS), :]) for q in range(PARTS)]
    g1 = gate(gates, 1)
    for number, block in enumerate(regroup([product(part, g0, 1, 0) for part in parts])):
        columns = slice(number * LANES, (number + 1) * LANES)
        high, low = halves(block)
        s1_high[:, columns], s1_low[:, columns] = high, low
        s2_high[:, columns], s2_low[:, columns] = halves(product((high, low), g1, 1, 0))
    g2 = gate(gates, 2)
    for e in range(s2_high.shape[0] // LANES):
        rows = slice(e * LANES, (e + 1) * LANES)
        s3 = product(g2, (s2_high[rows, :], s2_low[rows, :]), 0, 0)
        for p, block in enumerate(regroup([columns_of(s3, number) for number in range(PARTS)])):
            nat[pl.ds(e * PARTS * LANES + p, LANES, stride=PARTS), :] = block
    for d in range(send.shape[0] // LOW):
        c = chunk_of(d)
        send[d * LOW : (d + 1) * LOW, :] = nat[c * LOW : (c + 1) * LOW, :]


def gate(gates, number):
    return gates[number], gates[gates.shape[0] // 2 + number]


def turn_kernel(z, gates, v, u4_high, u4_low, half4, half5, half6, scratch):
    bits = own_bits()
    g3 = gate(gates, 3)
    for block in range(z.shape[0] // LANES):
        rows = slice(block * LANES, (block + 1) * LANES)
        scratch[rows, :] = product(g3, halves(z[rows, :]), 0, 0)
    for c in range(LOW):
        columns = slice(c * LANES, (c + 1) * LANES)
        u4_high[:, columns], u4_low[:, columns] = halves(scratch[pl.ds(c, LANES, stride=LOW), :])
    v[...] = product(gate(gates, 4), (u4_high[...], u4_low[...]), 0, 0)
    for out, k in ((half4, 4), (half5, 5), (half6, 6)):
        size = 1 << k
        for j in range(LANES // (2 * size)):
            start = pl.multiple_of(j * 2 * size + (1 - bits[k - 3]) * size, size)
            out[j * size : (j + 1) * size, :] = v[pl.ds(start, size), :]


def weight(coef, mask, number):
    return coef[number] * mask[number].astype(F32)


def pair_matrix(low, high, scale):
    rows = lax.broadcasted_iota(jnp.int32, (LANES, LANES), 0)
    columns = lax.broadcasted_iota(jnp.int32, (LANES, LANES), 1)
    active = (((rows >> low) ^ (rows >> high)) & 1) == 1
    return jnp.where(active & ((rows ^ columns) == ((1 << low) | (1 << high))), scale, 0.0)


def local_hops_kernel(v, z, coef, mask, out, z_high, z_low):
    z_high[...], z_low[...] = halves(z[...])
    lane_chain = sum(pair_matrix(LANE_BIT[k], LANE_BIT[k + 1], weight(coef, mask, k)) for k in range(6))
    top_chain = sum(pair_matrix(k, k + 1, weight(coef, mask, CHAIN_FIRST + k)) for k in range(6))
    lane_chain, top_chain = halves(lane_chain), halves(top_chain)
    rows = lax.broadcasted_iota(jnp.int32, (LANES, LANES), 0)
    columns = lax.broadcasted_iota(jnp.int32, (LANES, LANES), 1)
    rungs = []
    for k in range(3):
        scale = weight(coef, mask, RUNG_FIRST + k)
        paired = (rows ^ columns) == (1 << k)
        rungs.append([halves(jnp.where(paired & (((rows >> k) & 1) == 1 - c), scale, 0.0)) for c in range(2)])
    blocks = [v[:, c * LANES : (c + 1) * LANES] for c in range(LOW)]
    parts = [halves(block) for block in blocks]
    for c in range(LOW):
        total = product(parts[c], lane_chain, 1, 0) + product(top_chain, parts[c], 1, 0)
        for k in range(3):
            total = total + product(rungs[k][(c >> k) & 1], parts[c ^ (1 << k)], 1, 0)
        step = 1 << LANE_BIT[6]
        moved = pltpu.roll(blocks[c ^ 1], LANES - step if c & 1 else step, 1)
        wanted = ((columns >> LANE_BIT[6]) & 1) == 1 - (c & 1)
        total = total + jnp.where(wanted, weight(coef, mask, 6) * moved, 0.0)
        for k in range(2):
            if (c >> k) & 1 != (c >> (k + 1)) & 1:
                total = total + weight(coef, mask, 7 + k) * blocks[c ^ (3 << k)]
        out[:, c * LANES : (c + 1) * LANES] = total


def return_kernel(
    hops, other, half4, half5, half6, coef, mask, u4_high, u4_low, z_high, z_low, gates, send, grams, lam, scratch
):
    bits = own_bits()
    lam[...] = hops[...]
    wide = lam.shape[1] // 2
    to = pl.multiple_of((1 - bits[0]) * wide, wide)
    source = pl.multiple_of(bits[0] * wide, wide)
    lam[:, pl.ds(to, wide)] += weight(coef, mask, 9) * other[:, pl.ds(source, wide)]
    for j in range(LANES // 16):
        to = pl.multiple_of(j * 16 + (1 - bits[0]) * 8, 8)
        source = pl.multiple_of(j * 16 + bits[0] * 8, 8)
        lam[pl.ds(to, 8), :] += weight(coef, mask, RUNG_FIRST + 3) * other[pl.ds(source, 8), :]
    for half, k in ((half4, 4), (half5, 5), (half6, 6)):
        size = 1 << k
        for j in range(LANES // (2 * size)):
            to = pl.multiple_of(j * 2 * size + (1 - bits[k - 3]) * size, size)
            lam[pl.ds(to, size), :] += weight(coef, mask, RUNG_FIRST + k) * half[j * size : (j + 1) * size, :]
    lam5 = halves(lam[...])
    grams[1] = product(lam5, (u4_high[...], u4_low[...]), 1, 1)
    lam4 = product(gate(gates, 4), lam5, 1, 0)
    for c in range(LOW):
        scratch[pl.ds(c, LANES, stride=LOW), :] = lam4[:, c * LANES : (c + 1) * LANES]
    g3 = gate(gates, 3)
    gram = jnp.zeros((LANES, LANES), F32)
    for block in range(z_high.shape[0] // LANES):
        rows = slice(block * LANES, (block + 1) * LANES)
        inner = halves(scratch[rows, :])
        gram = gram + product(inner, (z_high[rows, :], z_low[rows, :]), 1, 1)
        send[rows, :] = product(g3, inner, 1, 0)
    grams[0] = gram


def backward_kernel(
    received, x, s1_high, s1_low, s2_high, s2_low, gates, upper, lam1_high, lam1_low, own, away, nat, pack
):
    for d in range(received.shape[0] // LOW):
        c = chunk_of(d)
        nat[c * LOW : (c + 1) * LOW, :] = received[d * LOW : (d + 1) * LOW, :]
    count = x.shape[0] // PARTS
    g2 = gate(gates, 2)
    gram2 = jnp.zeros((LANES, LANES), F32)
    pieces = []
    for e in range(count // LANES):
        rows = slice(e * LANES, (e + 1) * LANES)
        blocks = [nat[pl.ds(e * PARTS * LANES + p, LANES, stride=PARTS), :] for p in range(PARTS)]
        lam3 = halves(jnp.concatenate(regroup(blocks), axis=1))
        gram2 = gram2 + product(lam3, (s2_high[rows, :], s2_low[rows, :]), 1, 1)
        pieces.append(product(g2, lam3, 1, 0))
    lam2 = halves(jnp.concatenate(pieces, axis=0))
    g1 = gate(gates, 1)
    gram1 = jnp.zeros((LANES, LANES), F32)
    blocks = []
    for number in range(PARTS):
        inner = (columns_of(lam2[0], number), columns_of(lam2[1], number))
        gram1 = gram1 + product(inner, (columns_of(s1_high, number), columns_of(s1_low, number)), 0, 0)
        blocks.append(product(inner, g1, 1, 1))
    gram0 = jnp.zeros((LANES, LANES), F32)
    for q, block in enumerate(regroup(blocks)):
        columns = slice(q * LANES, (q + 1) * LANES)
        inner = halves(block)
        lam1_high[:, columns], lam1_low[:, columns] = inner
        gram0 = gram0 + product(inner, halves(x[pl.ds(q, count, stride=PARTS), :]), 0, 0)
    order = lane_order()
    dot = functools.partial(jnp.dot, preferred_element_type=F32)
    high, low = halves(gram0)
    gram0 = dot(order, high) + dot(order, low)
    size = LANES // (CORES * NEAR)
    for k, gram in enumerate((gram0, gram1, gram2, upper[0], upper[1])):
        for d in range(CORES * NEAR):
            start = (d * 5 + k) * size
            pack[start : start + size, :] = gram[d * size : (d + 1) * size, :]
    core = own_bits()[0]
    rows = own.shape[0]
    own[...] = pack[pl.ds(pl.multiple_of(core * rows, rows), rows), :]
    away[...] = pack[pl.ds(pl.multiple_of((1 - core) * rows, rows), rows), :]


def finish_kernel(lam1_high, lam1_low, gates, adjoint, done):
    done[...] = jnp.zeros_like(done)
    g0 = gate(gates, 0)
    count = lam1_high.shape[0]
    for q in range(PARTS):
        part = slice(q * LANES, (q + 1) * LANES)
        adjoint[pl.ds(q, count, stride=PARTS), :] = product((lam1_high[:, part], lam1_low[:, part]), g0, 1, 1)


def merge_kernel(own, other, done, merged):
    merged[...] = own[...] + other[...]


def sum_and_copy_kernel(received, pack, *, sources, factor):
    size = received.shape[0] // sources
    value = received[0:size, :]
    for d in range(1, sources):
        value = value + received[d * size : (d + 1) * size, :]
    for d in range(pack.shape[0] // size):
        pack[d * size : (d + 1) * size, :] = factor * value


def gather_kernel(own, other, grads):
    size = LANES // (CORES * NEAR)
    core = own_bits()[0]
    for source, half in ((own, core), (other, 1 - core)):
        for d in range(NEAR):
            row = pl.multiple_of((half * NEAR + d) * size, size)
            for k in range(5):
                start = (d * 5 + k) * size
                grads[k, pl.ds(row, size), :] = source[start : start + size, :]


def call(kernel, outs, specs, scratch=(), name=None):
    made = pl.pallas_call(
        kernel,
        out_shape=[
            jax.ShapeDtypeStruct(out[0], out[1]) if len(out) > 2 else pltpu.VMEM(out[0], out[1]) for out in outs
        ],
        in_specs=specs,
        out_specs=[VMEM] * len(outs),
        scratch_shapes=list(scratch),
        compiler_params=pltpu.CompilerParams(vmem_limit_bytes=24 << 20),
        name=name,
    )

    def run(*operands):
        kept = [
            operand
            if spec is SMEM
            else pltpu.with_memory_space_constraint(operand, pltpu.HBM if spec is FAR else pltpu.VMEM)
            for operand, spec in zip(operands, specs)
        ]
        return made(*kept)

    return run


def exchange(rows, axes):
    devices = lax.axis_size(axes)
    shaped = rows.reshape(devices, rows.shape[0] // devices, 1, rows.shape[1])
    return lax.all_to_all(shaped, axes, split_axis=0, concat_axis=0, tiled=True).reshape(rows.shape)


def swapped(value, flip):
    return lax.ppermute(value, AMP, [(i, i ^ flip) for i in range(lax.axis_size(AMP))])


def on_device(initial_state, gate_angles, gate_pairs, hop_coef, hop_mask):
    devices = lax.axis_size(AMP)
    middle = initial_state.shape[1]
    x = initial_state.reshape(middle, LANES)
    blocks, rotations = gate_angles.shape
    wide = (middle // PARTS, PARTS * LANES)
    turned = (devices, LOW * LANES)
    half = (devices // 2, LOW * LANES)
    level = pltpu.VMEM((blocks, rotations // 2, LANES, LANES), BF16)
    flat = pltpu.VMEM((middle, LANES), F32)

    send, x_near, s1_high, s1_low, s2_high, s2_low, gates = call(
        forward_kernel,
        [((middle, LANES), F32)] * 2
        + [(wide, BF16)] * 4
        + [((2 * blocks, LANES, LANES), BF16)],
        [FAR] * 3,
        [
            level,
            level,
            flat,
            pltpu.VMEM(gate_angles.shape, F32),
            pltpu.SMEM((blocks, 2, rotations), jnp.int32),
            pltpu.SemaphoreType.DMA((3,)),
        ],
        "forward",
    )(gate_angles, jnp.swapaxes(gate_pairs, 1, 2), x)
    z = exchange(send, AMP)
    v, u4_high, u4_low, half4, half5, half6 = call(
        turn_kernel,
        [(turned, F32), (turned, BF16), (turned, BF16), (half, F32), (half, F32), (half, F32)],
        [VMEM, VMEM],
        [flat],
        "turn",
    )(z, gates)
    half4, half5, half6 = swapped(half4, 2), swapped(half5, 6), swapped(half6, 8)
    other = swapped(v, 1)
    hops, z_high, z_low = call(
        local_hops_kernel,
        [(turned, F32), ((middle, LANES), BF16), ((middle, LANES), BF16)],
        [VMEM, VMEM, SMEM, SMEM],
        (),
        "hops",
    )(v, z, hop_coef, hop_mask)
    send, upper = call(
        return_kernel,
        [((middle, LANES), F32), ((2, LANES, LANES), F32)],
        [VMEM] * 5 + [SMEM] * 2 + [VMEM] * 5,
        [pltpu.VMEM(turned, F32), flat],
        "back",
    )(hops, other, half4, half5, half6, hop_coef, hop_mask, u4_high, u4_low, z_high, z_low, gates)
    received = exchange(send, AMP)
    part = ((5 * LANES // CORES, LANES), F32)
    lam1_high, lam1_low, own, away = call(
        backward_kernel,
        [(wide, BF16), (wide, BF16), part, part],
        [VMEM] * 8,
        [flat, pltpu.VMEM((5 * LANES, LANES), F32)],
        "backward",
    )(received, x_near, s1_high, s1_low, s2_high, s2_low, gates, upper)
    away = swapped(away, 1)
    adjoint, done = call(
        finish_kernel, [((middle, LANES), F32, True), ((LOW, LANES), F32)], [VMEM] * 3, (), "finish"
    )(lam1_high, lam1_low, gates)
    (partial,) = call(merge_kernel, [part], [VMEM] * 3, (), "merge")(own, away, done)
    far = devices // (CORES * NEAR)
    rows = ((far * part[0][0] // NEAR, LANES), F32)
    near_sum = functools.partial(sum_and_copy_kernel, sources=NEAR, factor=1.0)
    (partial,) = call(near_sum, [rows], [VMEM], (), "near")(exchange(partial, "near"))
    far_sum = functools.partial(sum_and_copy_kernel, sources=far, factor=2.0 / (devices * middle))
    (sums,) = call(far_sum, [part], [VMEM], (), "far")(exchange(partial, "far"))
    sums = exchange(sums, "near")
    (grads,) = call(gather_kernel, [((blocks, LANES, LANES), F32, True)], [VMEM] * 2, (), "gather")(sums, swapped(sums, 1))
    return adjoint.reshape(initial_state.shape), grads


def solution(mesh):
    runs, amp = mesh.shape["runs"], mesh.shape["amp"]
    split = Mesh(mesh.devices.reshape(runs, amp // (NEAR * CORES), NEAR, CORES), ("runs",) + AMP)
    return jax.shard_map(
        on_device,
        mesh=split,
        in_specs=(P(("runs",) + AMP, None, None), P("runs", None), P(), P(), P()),
        out_specs=(P(("runs",) + AMP, None, None), P("runs", None, None)),
        check_vma=False,
    )
```
